32 devices in a mesh: batch: 1 (over z), col: 4 (over y), row: 8 (over x, core).
Axes of the slice: x: 4, y: 4, z: 1, core: 2. Of those that a mesh axis runs over, the one named last changes fastest.
The devices are a block of a 4x4x8 slice.
Arguments:
- z_one: bfloat16 [1024, 1024, 64], P(('batch', 'row'), 'col')
- z_two: bfloat16 [1024, 1024, 64], P(('batch', 'row'), 'col')
- mask_one: int32 [1024, 1024], P(('batch', 'row'), 'col')
- mask_two: int32 [1024, 1024], P(('batch', 'row'), 'col')
- ln_in_scale: bfloat16 [64], replicated
- w_a: bfloat16 [64, 64], replicated
- w_a_gate: bfloat16 [64, 64], replicated
- w_b: bfloat16 [64, 64], replicated
- w_b_gate: bfloat16 [64, 64], replicated
- w_gate: bfloat16 [64, 64], replicated
- w_out: bfloat16 [64, 64], replicated
- ln_out_scale: bfloat16 [64], replicated
Outputs:
- output 1: bfloat16 [1024, 1024, 64], P(('batch', 'row'), 'col')
- output 2: bfloat16 [1024, 1024, 64], P(('batch', 'row'), 'col')
All inputs are finite; a program needn't handle non-finite values.
Results may differ from the reference program's by a relative error of at most 0.001.
Values are sent between devices in bfloat16 or wider.
A program may use at most 768 MiB of HBM per device.

```python
import jax
import jax.numpy as jnp
from jax import lax

NRES = 1024
CZ = 64
CHID = 64
ROW_BLOCK = 128


def layer_norm(values, scale):
    row_mean = jnp.mean(values, axis=-1, keepdims=True)
    centered = values - row_mean
    variance = jnp.mean(centered * centered, axis=-1, keepdims=True)
    return centered * lax.rsqrt(variance + 1e-5) * scale.astype(jnp.float32)


def linear(normed, weight):
    flat = normed.reshape(-1, normed.shape[-1])
    result = jnp.dot(flat, weight, preferred_element_type=jnp.float32)
    return result.reshape(normed.shape[:-1] + (weight.shape[1],))


def one_crop(pair, mask, ln_in_scale, w_a, w_a_gate, w_b, w_b_gate, w_gate, w_out, ln_out_scale):
    block_count = NRES // ROW_BLOCK
    pair_blocks = pair.reshape(block_count, ROW_BLOCK, NRES, CZ)
    mask_blocks = mask.reshape(block_count, ROW_BLOCK, NRES)

    def project(block):
        pair_blk, mask_blk = block
        normed = layer_norm(pair_blk.astype(jnp.float32), ln_in_scale).astype(jnp.bfloat16)
        mask_val = mask_blk.astype(jnp.float32)[:, :, None]
        left = mask_val * jax.nn.sigmoid(linear(normed, w_a_gate)) * linear(normed, w_a)
        right = mask_val * jax.nn.sigmoid(linear(normed, w_b_gate)) * linear(normed, w_b)
        return left.astype(jnp.bfloat16), right.astype(jnp.bfloat16)

    left_all, right_all = lax.map(project, (pair_blocks, mask_blocks))
    right_major = jnp.transpose(right_all.reshape(NRES, NRES, CHID).astype(jnp.float32), (2, 0, 1))

    def finish(block):
        pair_blk, left_blk = block
        normed = layer_norm(pair_blk.astype(jnp.float32), ln_in_scale).astype(jnp.bfloat16)
        gate = jax.nn.sigmoid(linear(normed, w_gate))
        left_major = jnp.transpose(left_blk.astype(jnp.float32), (2, 0, 1))
        contracted = jnp.einsum('cik,cjk->ijc', left_major, right_major)
        normed_out = layer_norm(contracted, ln_out_scale).astype(jnp.bfloat16)
        update = linear(normed_out, w_out)
        return (pair_blk.astype(jnp.float32) + gate * update).astype(jnp.bfloat16)

    out_blocks = lax.map(finish, (pair_blocks, left_all))
    return out_blocks.reshape(NRES, NRES, CZ)


def setup_inputs(seed: int = 0, part: int = 0) -> dict:
    root = jax.random.key(seed)
    shared_key, crop_base = jax.random.split(root)
    crop_keys = jax.random.split(jax.random.fold_in(crop_base, part), 4)
    weight_keys = jax.random.split(shared_key, 8)

    def pair_draw(key_in):
        return jax.random.normal(key_in, (NRES, NRES, CZ), jnp.float32).astype(jnp.bfloat16)

    def mask_draw(key_in):
        valid = (jax.random.randint(key_in, (NRES,), 0, 10) != 0).astype(jnp.int32)
        return valid[:, None] * valid[None, :]

    def weight_draw(key_in, fan_in, fan_out):
        values = jax.random.normal(key_in, (fan_in, fan_out), jnp.float32) * fan_in ** -0.5
        return values.astype(jnp.bfloat16)

    def scale_draw(key_in, width):
        return jax.random.uniform(key_in, (width,), jnp.float32, 0.5, 1.5).astype(jnp.bfloat16)

    return {
        'z_one': pair_draw(crop_keys[0]),
        'z_two': pair_draw(crop_keys[1]),
        'mask_one': mask_draw(crop_keys[2]),
        'mask_two': mask_draw(crop_keys[3]),
        'ln_in_scale': scale_draw(weight_keys[0], CZ),
        'w_a': weight_draw(weight_keys[1], CZ, CHID),
        'w_a_gate': weight_draw(weight_keys[2], CZ, CHID),
        'w_b': weight_draw(weight_keys[3], CZ, CHID),
        'w_b_gate': weight_draw(weight_keys[4], CZ, CHID),
        'w_gate': weight_draw(weight_keys[5], CZ, CZ),
        'w_out': weight_draw(weight_keys[6], CHID, CZ),
        'ln_out_scale': scale_draw(weight_keys[7], CHID),
    }


def reference(z_one, z_two, mask_one, mask_two, ln_in_scale, w_a, w_a_gate, w_b, w_b_gate, w_gate, w_out, ln_out_scale):
    out_one = one_crop(z_one, mask_one, ln_in_scale, w_a, w_a_gate, w_b, w_b_gate, w_gate, w_out, ln_out_scale)
    out_two = one_crop(z_two, mask_two, ln_in_scale, w_a, w_a_gate, w_b, w_b_gate, w_gate, w_out, ln_out_scale)
    return (out_one, out_two)
```

```python
import functools
import jax
import jax.numpy as jnp
from jax import lax
from jax.experimental import pallas as pl
from jax.experimental.pallas import tpu as pltpu
from jax.sharding import PartitionSpec as P

MESH = pl.DeviceIdType.MESH
F32 = jnp.float32
BF16 = jnp.bfloat16
EPS = 1e-5
STEPS = 2
ROWS = 16
VMEM_LIMIT = 60 * 1024 * 1024


def normalise_row(row, scale_col):
    values = row.astype(F32)
    count = values.shape[0]
    mean = jnp.sum(values, axis=0, keepdims=True) / count
    centered = values - mean
    variance = jnp.sum(centered * centered, axis=0, keepdims=True) / count
    return (centered * lax.rsqrt(variance + EPS) * scale_col).astype(BF16)


def project_kernel(z_ref, mask_ref, scale_ref, w_ref, a_ref, b_ref, sa, sb):
    rows, ch, cols = z_ref.shape
    hid = sa.shape[1]
    scale_col = scale_ref[...]

    def one_row(i, carry):
        normed = normalise_row(z_ref[i], scale_col)
        prod = jnp.dot(w_ref[...], normed, preferred_element_type=F32)
        mask = mask_ref[pl.ds(i, 1), :].astype(F32)
        sa[i] = mask * jax.nn.sigmoid(prod[:hid]) * prod[hid:2 * hid]
        sb[i] = mask * jax.nn.sigmoid(prod[2 * hid:3 * hid]) * prod[3 * hid:]
        return carry

    lax.fori_loop(0, rows, one_row, 0, unroll=2)
    for e in range(0, hid, 8):
        a_ref[e:e + 8] = jnp.transpose(sa[:, e:e + 8, :], (1, 0, 2)).astype(BF16)
        b_ref[0, e:e + 8] = jnp.transpose(sb[:, e:e + 8, :], (1, 0, 2)).astype(BF16)


def project(z_t, mask, scale_col, w_in):
    rows, ch, cols = z_t.shape
    hid = w_in.shape[0] // 4
    chunk = min(ROWS, rows // STEPS)
    per_step = rows // STEPS // chunk
    return pl.pallas_call(
        project_kernel,
        grid=(rows // chunk,),
        in_specs=[
            pl.BlockSpec((chunk, ch, cols), lambda i: (i, 0, 0)),
            pl.BlockSpec((chunk, cols), lambda i: (i, 0)),
            pl.BlockSpec((ch, 1), lambda i: (0, 0)),
            pl.BlockSpec((4 * hid, ch), lambda i: (0, 0)),
        ],
        out_specs=[
            pl.BlockSpec((hid, chunk, cols), lambda i: (0, i, 0)),
            pl.BlockSpec((1, hid, chunk, cols), lambda i: (i // per_step, 0, i % per_step, 0)),
        ],
        out_shape=[
            jax.ShapeDtypeStruct((hid, rows, cols), BF16),
            jax.ShapeDtypeStruct((STEPS, hid, rows // STEPS, cols), BF16),
        ],
        scratch_shapes=[pltpu.VMEM((chunk, hid, cols), F32), pltpu.VMEM((chunk, hid, cols), F32)],
        cost_estimate=pl.CostEstimate(flops=2 * rows * cols * ch * 4 * hid, bytes_accessed=rows * cols * ch * 6, transcendentals=rows * cols * hid * 2),
        name="project",
    )(z_t, mask, scale_col, w_in)


def finish_kernel(z_ref, n_ref, scale_ref, w_gate_ref, w_out_ref, o_ref, sn):
    rows, ch, cols = z_ref.shape
    steps, hid, _, lanes = n_ref.shape
    cores = cols // (lanes // 2 * steps) if steps > 1 else 1
    part = lanes // cores
    scale_col = scale_ref[...]
    for e in range(0, hid, 8):
        pieces = [jnp.transpose(n_ref[s, e:e + 8].astype(F32), (1, 0, 2)) for s in range(steps)]
        order = [pieces[s][:, :, r * part:(r + 1) * part] for r in range(cores) for s in range(steps)]
        sn[:, e:e + 8, :] = jnp.concatenate(order, axis=2)

    def one_row(i, carry):
        row = z_ref[i]
        normed = normalise_row(row, scale_col)
        gate = jax.nn.sigmoid(jnp.dot(w_gate_ref[...], normed, preferred_element_type=F32))
        update = jnp.dot(w_out_ref[...], sn[i].astype(BF16), preferred_element_type=F32)
        o_ref[i] = (row.astype(F32) + gate * update).astype(BF16)
        return carry

    lax.fori_loop(0, rows, one_row, 0, unroll=2)


def finish(z_t, n_all, which, scale_col, w_gate_t, w_out_t):
    rows, ch, cols = z_t.shape
    steps = STEPS
    hid, lanes = n_all.shape[1], n_all.shape[3]
    chunk = min(ROWS, rows)
    return pl.pallas_call(
        finish_kernel,
        grid=(rows // chunk,),
        in_specs=[
            pl.BlockSpec((chunk, ch, cols), lambda i: (i, 0, 0)),
            pl.BlockSpec((steps, hid, chunk, lanes), lambda i: (which, 0, i, 0)),
            pl.BlockSpec((ch, 1), lambda i: (0, 0)),
            pl.BlockSpec((ch, ch), lambda i: (0, 0)),
            pl.BlockSpec((ch, hid), lambda i: (0, 0)),
        ],
        out_specs=pl.BlockSpec((chunk, ch, cols), lambda i: (i, 0, 0)),
        out_shape=jax.ShapeDtypeStruct((rows, ch, cols), BF16),
        scratch_shapes=[pltpu.VMEM((chunk, hid, cols), F32)],
        cost_estimate=pl.CostEstimate(flops=4 * rows * cols * ch * hid, bytes_accessed=rows * cols * ch * 6, transcendentals=rows * cols * ch * 2),
        name="finish",
    )(z_t, n_all, scale_col, w_gate_t, w_out_t)


def exchange_kernel(ny, nx, cores, a0, a1, b0, b1, scale_ref,
                    n_out, a_all, a_relay, by, b_relay, bx, bo, n_relay,
                    a_v, b_v, o_v, ssum, st, st_in, mr, mr_in, nv, send_sems, recv_sems, loc_sems):
    a_in, b_in = (a0, a1), (b0, b1)
    crops = 2
    cb = o_v.shape[1]
    rows = o_v.shape[2]
    lanes = o_v.shape[3]
    sub = lanes // cores
    hid = cb * ny
    half = cb // 2
    y = lax.axis_index("col")
    row_id = lax.axis_index("row")
    x, r = row_id // cores, row_id % cores
    yy = [lax.rem(y + d, ny) for d in range(ny)]
    xr = [lax.rem(x + e, nx) * cores + r for e in range(nx)]
    partner = x * cores + (cores - 1 - r)
    to_y = [{"col": yy[d]} for d in range(ny)]
    to_x = [{"row": xr[e]} for e in range(nx)]
    to_p = {"row": partner}

    barrier = pltpu.get_barrier_semaphore()
    peers = to_y[1:] + [to_x[1], to_x[nx - 1], to_p]
    for dev in peers:
        pl.semaphore_signal(barrier, inc=1, device_id=dev, device_id_type=MESH)
    pl.semaphore_wait(barrier, len(peers))

    count = [0]
    sent = []

    def send(src, dst, dev):
        k = count[0]
        count[0] += 1
        copy = pltpu.make_async_remote_copy(
            src_ref=src, dst_ref=dst, send_sem=send_sems.at[k], recv_sem=recv_sems.at[k],
            device_id=dev, device_id_type=MESH)
        copy.start()
        sent.append(copy)
        return copy

    class AllToAll:
        def __init__(self, piece, direct, relay, onward):
            self.piece, self.direct, self.relay, self.onward = piece, direct, relay, onward

        def start(self):
            far = self.piece(2)
            self.r0 = send(far.at[:half], self.relay.at[0], to_y[1])
            self.r1 = send(far.at[half:], self.relay.at[1], to_y[3])
            self.c1 = send(self.piece(1), self.direct(1), to_y[1])
            self.c3 = send(self.piece(3), self.direct(3), to_y[3])

        def forward(self):
            self.r0.wait_recv()
            self.f0 = send(self.relay.at[0], self.onward(0).at[:half], to_y[1])
            self.r1.wait_recv()
            self.f1 = send(self.relay.at[1], self.onward(1).at[half:], to_y[3])

        def wait(self, d):
            if d == 1:
                self.c3.wait_recv()
            elif d == 3:
                self.c1.wait_recv()
            else:
                self.f0.wait_recv()
                self.f1.wait_recv()

    def a_unit(t):
        return AllToAll(lambda d: a_in[t].at[yy[d]], lambda d: a_all.at[t, 3 - d], a_relay.at[t], lambda h: a_all.at[t, 1])

    def b_unit(q):
        t, s = divmod(q, STEPS)
        return AllToAll(lambda d: b_in[t].at[s, yy[d]], lambda d: by.at[q, 3 - d], b_relay.at[q], lambda h: by.at[q, 1])

    def n_unit(q):
        return AllToAll(lambda d: nv.at[q, d], lambda d: n_out.at[q, y], n_relay.at[q],
                        lambda h: n_out.at[q, yy[3] if h == 0 else yy[1]])

    last = crops * STEPS
    ua = [a_unit(t) for t in range(crops)]
    ub = [b_unit(q) for q in range(last)]
    un = [n_unit(q) for q in range(last)]

    def own_piece(q, e, d):
        t, s = divmod(q, STEPS)
        if e == 0:
            return b_in[t].at[s, y] if d == 0 else by.at[q, d - 1]
        return bx.at[q, e - 1, d]

    xp, xm, xf, dd = {}, {}, {}, {}

    def x_direct(q, d):
        piece = own_piece(q, 0, d)
        xp[q, d] = send(piece, bx.at[q, 2, d], to_x[1])
        xm[q, d] = send(piece, bx.at[q, 0, d], to_x[3])

    def x_forward(q, d):
        xp[q, d].wait_recv()
        f0 = send(bx.at[q, 2, d].at[:half], bx.at[q, 1, d].at[:half], to_x[1])
        xm[q, d].wait_recv()
        f1 = send(bx.at[q, 0, d].at[half:], bx.at[q, 1, d].at[half:], to_x[3])
        xf[q, d] = (f0, f1)
        cross(q, 3, d)
        cross(q, 1, d)

    def x_far(q, d):
        for f in xf[q, d]:
            f.wait_recv()
        cross(q, 2, d)

    def cross(q, e, d):
        dd[q, e, d] = send(own_piece(q, e, d), bo.at[q, e, d], to_p)

    def local(src, dst, k):
        copy = pltpu.make_async_copy(src, dst, loc_sems.at[k])
        copy.start()
        return copy

    def load_b(q):
        copies = []
        for e in range(nx):
            for d in range(ny):
                dst = pl.ds(pl.multiple_of(e * lanes + r * sub, sub), sub)
                copies.append(local(own_piece(q, e, d), b_v.at[d, :, dst, :], len(copies)))
        for e in range(nx):
            for d in range(ny):
                dd[q, e, d].wait_recv()
                dst = pl.ds(pl.multiple_of(e * lanes + (cores - 1 - r) * sub, sub), sub)
                copies.append(local(bo.at[q, e, d], b_v.at[d, :, dst, :], len(copies)))
        return copies

    def load_a(t):
        base = 2 * nx * ny
        copies = [local(a_in[t].at[y], a_v.at[0], base)]
        for d in (1, 3, 2):
            ua[t].wait(d)
            copies.append(local(a_all.at[t, d - 1], a_v.at[d], base + d))
        return copies

    def contract(q):
        ssum[...] = jnp.zeros_like(ssum)

        def channel(c, carry):
            acc = None
            for d in range(ny):
                term = lax.dot_general(a_v[d, c], b_v[d, c], (((1,), (1,)), ((), ())), preferred_element_type=F32)
                acc = term if acc is None else acc + term
            for e in range(nx):
                part = acc[:, e * lanes:(e + 1) * lanes]
                o_v[e, c] = part
                ssum[e] += part
            return carry

        lax.fori_loop(0, cb, channel, 0)
        block = min(16, rows)

        def squares(k, carry):
            rs = pl.ds(pl.multiple_of(k * block, block), block)
            for e in range(nx):
                total = ssum[e, rs, :]
                mean = total * (1.0 / cb)
                acc = jnp.zeros_like(mean)
                for c in range(cb):
                    diff = o_v[e, c, rs, :] - mean
                    acc = acc + diff * diff
                st[q, e, 0, rs, :] = total
                st[q, e, 1, rs, :] = acc
            return carry

        lax.fori_loop(0, rows // block, squares, 0)

    e_of = [lax.rem(y + d + nx - x, nx) for d in range(ny)]
    stat, back = {}, {}

    def stats_send(q):
        for d in (2, 1, 3):
            stat[q, d] = send(st.at[q, e_of[d]], st_in.at[q, 3 - d], to_y[d])

    def stats_reduce(q):
        for d in (1, 3, 2):
            stat[q, d].wait_recv()
        mine = st[q, e_of[0]]
        parts = [mine] + [st_in[q, k] for k in range(ny - 1)]
        mean = (parts[0][0] + parts[1][0] + parts[2][0] + parts[3][0]) * (1.0 / hid)
        m2 = jnp.zeros_like(mean)
        for part in parts:
            diff = part[0] * (1.0 / cb) - mean
            m2 = m2 + part[1] + cb * (diff * diff)
        mr[q, 0] = mean
        mr[q, 1] = lax.rsqrt(m2 * (1.0 / hid) + EPS)

    def stats_back(q):
        for d in (2, 1, 3):
            back[q, d] = send(mr.at[q], mr_in.at[q, 3 - d], to_y[d])

    def apply_norm(q):
        for d in (0, 1, 3, 2):
            if d:
                back[q, 4 - d].wait_recv()
            mean = mr[q, 0] if d == 0 else mr_in[q, d - 1, 0]
            rstd = mr[q, 1] if d == 0 else mr_in[q, d - 1, 1]
            e = e_of[d]

            def channel(c, carry, mean=mean, rstd=rstd, e=e, d=d):
                nv[q, d, c] = ((o_v[e, c] - mean) * rstd * scale_ref[y * cb + c]).astype(BF16)
                return carry

            lax.fori_loop(0, cb, channel, 0)

    keep = []

    def n_send(q):
        keep.append(local(nv.at[q, 0], n_out.at[q, y], 2 * nx * ny + ny + q))
        un[q].start()

    ub[0].start()
    x_direct(0, 0)
    ua[0].start()
    ub[0].forward()
    for q in range(last + 1):
        t = q // STEPS
        if q < last:
            for d in (1, 3, 2):
                ub[q].wait(d)
                x_direct(q, d)
            for d in (0, 1, 3, 2):
                cross(q, 0, d)
        if q > 0:
            if (q - 1) % STEPS == 0:
                for copy in load_a((q - 1) // STEPS):
                    copy.wait()
            for copy in pending:
                copy.wait()
            contract(q - 1)
            stats_send(q - 1)
        if q + 1 < last:
            ub[q + 1].start()
            if (q + 1) % STEPS == 0:
                ua[(q + 1) // STEPS].start()
        if q < last and q % STEPS == 0:
            ua[t].forward()
        if q > 0:
            stats_reduce(q - 1)
            stats_back(q - 1)
        if q > 1:
            un[q - 2].forward()
        if q < last:
            x_forward(q, 0)
        if q > 0:
            apply_norm(q - 1)
            n_send(q - 1)
        if q < last:
            for d in (1, 3):
                x_forward(q, d)
            if q + 1 < last:
                ub[q + 1].forward()
                x_direct(q + 1, 0)
            x_forward(q, 2)
            for d in (0, 1, 3, 2):
                x_far(q, d)
            pending = load_b(q)
    un[last - 1].forward()
    for q in range(last):
        for d in (1, 3, 2):
            un[q].wait(d)
        keep[q].wait()
    for copy in sent:
        copy.wait_send()


def exchange(a_pair, b_pair, scale, ny, nx, cores):
    hid, rows, cols = a_pair[0].shape
    cb = hid // ny
    sub = rows // STEPS
    lanes = cores * sub
    q = 2 * STEPS
    a_pair = [a.reshape(ny, cb, rows, cols) for a in a_pair]
    b_pair = [b.reshape(STEPS, ny, cb, sub, cols) for b in b_pair]
    any_spec = pl.BlockSpec(memory_space=pl.ANY)

    def hbm(*shape):
        return jax.ShapeDtypeStruct(shape, BF16)

    sends = 2 * 6 + q * (6 + 4 * ny + nx * ny + 3 + 3 + 6)
    outs = pl.pallas_call(
        functools.partial(exchange_kernel, ny, nx, cores),
        in_specs=[any_spec] * 4 + [pl.BlockSpec(memory_space=pltpu.SMEM)],
        out_specs=[any_spec] * 8,
        out_shape=[
            hbm(q, ny, cb, rows, lanes),
            hbm(2, ny - 1, cb, rows, cols),
            hbm(2, 2, cb // 2, rows, cols),
            hbm(q, ny - 1, cb, sub, cols),
            hbm(q, 2, cb // 2, sub, cols),
            hbm(q, nx - 1, ny, cb, sub, cols),
            hbm(q, nx, ny, cb, sub, cols),
            hbm(q, 2, cb // 2, rows, lanes),
        ],
        scratch_shapes=[
            pltpu.VMEM((ny, cb, rows, cols), BF16),
            pltpu.VMEM((ny, cb, nx * lanes, cols), BF16),
            pltpu.VMEM((nx, cb, rows, lanes), F32),
            pltpu.VMEM((nx, rows, lanes), F32),
            pltpu.VMEM((q, nx, 2, rows, lanes), F32),
            pltpu.VMEM((q, ny - 1, 2, rows, lanes), F32),
            pltpu.VMEM((q, 2, rows, lanes), F32),
            pltpu.VMEM((q, ny - 1, 2, rows, lanes), F32),
            pltpu.VMEM((q, ny, cb, rows, lanes), BF16),
            pltpu.SemaphoreType.DMA((sends,)),
            pltpu.SemaphoreType.DMA((sends,)),
            pltpu.SemaphoreType.DMA((2 * nx * ny + ny + q,)),
        ],
        compiler_params=pltpu.CompilerParams(collective_id=0, has_side_effects=True, vmem_limit_bytes=VMEM_LIMIT),
        cost_estimate=pl.CostEstimate(flops=4 * rows * cols * hid * nx * cols, bytes_accessed=200000000, transcendentals=0),
        name="exchange",
    )(*a_pair, *b_pair, scale)
    return outs[0].reshape(q, hid, rows, lanes)


def solution(mesh):
    row_count = mesh.shape['row']
    col_count = mesh.shape['col']
    cores = row_count // col_count
    nx = row_count // cores
    pair_spec = P(('batch', 'row'), 'col', None)
    mask_spec = P(('batch', 'row'), 'col')
    replicated = P()

    def device_fn(z_one, z_two, mask_one, mask_two, ln_in_scale, w_a, w_a_gate, w_b, w_b_gate, w_gate, w_out, ln_out_scale):
        in_col = ln_in_scale.astype(F32)[:, None]
        w_in = jnp.concatenate([w_a_gate, w_a, w_b_gate, w_b], axis=1).T
        crops = [jnp.transpose(z, (0, 2, 1)) for z in (z_one, z_two)]
        ab = [project(z, m, in_col, w_in) for z, m in zip(crops, (mask_one, mask_two))]
        n_all = exchange([p[0] for p in ab], [p[1] for p in ab], ln_out_scale.astype(F32), col_count, nx, cores)
        outs = [finish(z, n_all, k, in_col, w_gate.T, w_out.T) for k, z in enumerate(crops)]
        return tuple(jnp.transpose(o, (0, 2, 1)) for o in outs)

    return jax.shard_map(
        device_fn,
        mesh=mesh,
        in_specs=(pair_spec, pair_spec, mask_spec, mask_spec) + (replicated,) * 8,
        out_specs=(pair_spec, pair_spec),
        check_vma=False,
    )
```

```python
import functools
import jax
import jax.numpy as jnp
from jax import lax
from jax.experimental import pallas as pl
from jax.experimental.pallas import tpu as pltpu
from jax.sharding import PartitionSpec as P

MESH = pl.DeviceIdType.MESH
F32 = jnp.float32
BF16 = jnp.bfloat16
EPS = 1e-5
STEPS = 2
ROWS = 16
VMEM_LIMIT = 60 * 1024 * 1024
ORDER = (
    ('proj',), ('proj',), ('bx', 0), ('b_start', 0), ('proj',), ('proj',), ('b_fwd', 0), ('bx', 1), ('proj',), ('xfwd', 0),
    ('b_start', 1), ('proj',), ('proj',), ('xfwd', 1), ('proj',), ('b_fwd', 1), ('xfar', 0), ('bx', 0), ('xfar', 1),
    ('b_start', 2), ('bx', 0), ('xfwd', 0), ('b_fwd', 2), ('xfwd', 0), ('a_relay', 0), ('xfar', 0), ('bx', 0), ('xfar', 0),
    ('a_dir', 0), ('load', 0), ('bx', 1), ('a_fwd', 0), ('xfwd', 0), ('xfwd', 1), ('a_dir', 0), ('xfar', 0), ('bx', 1),
    ('load2', 0), ('xfar', 1), ('b_start', 3), ('bx', 1), ('xfwd', 1), ('load_a', 0), ('con', 0), ('b_fwd', 3), ('con2', 0),
    ('bx', 2), ('xfwd', 1), ('a_relay', 1), ('xfar', 1), ('load', 1), ('rs2', 0), ('xfwd', 2), ('con', 1), ('a_fwd', 1),
    ('xfar', 1), ('bx', 2), ('red', 0), ('load2', 1), ('xfar', 2), ('con2', 1), ('a_dir', 1), ('bx', 2), ('xfwd', 2), ('ag2', 0),
    ('rs2', 1), ('xfwd', 2), ('norm', 0), ('xfar', 2), ('bx', 2), ('xfar', 2), ('a_dir', 1), ('load', 2), ('red', 1), ('bx', 3),
    ('xfwd', 2), ('nfwd', 0), ('xfwd', 3), ('load_a', 1), ('ag2', 1), ('xfar', 2), ('bx', 3), ('load2', 2), ('nwait', 0),
    ('xfar', 3), ('norm', 1), ('con', 2), ('bx', 3), ('con2', 2), ('xfwd', 3), ('nfwd', 1), ('rs2', 2), ('xfwd', 3),
    ('nwait', 1), ('red', 2), ('xfar', 3), ('bx', 3), ('ag2', 2), ('xfar', 3), ('norm', 2), ('load', 3), ('fin',), ('fin',),
    ('xfwd', 3), ('con', 3), ('xfar', 3), ('nfwd', 2), ('load2', 3), ('con2', 3), ('nwait', 2), ('fin',), ('rs2', 3), ('fin',),
    ('red', 3), ('ag2', 3), ('norm', 3), ('nfwd', 3), ('nwait', 3),
)


def normalise_row(row, scale):
    values = row.astype(F32)
    count = values.shape[0]
    mean = jnp.sum(values, axis=0, keepdims=True) / count
    centered = values - mean
    variance = jnp.sum(centered * centered, axis=0, keepdims=True) / count
    return (centered * lax.rsqrt(variance + EPS) * scale).astype(BF16)


def transposed(ref):
    return jnp.transpose(ref[...].astype(F32), (1, 0)).astype(BF16)


def store_weights(in_ref, w_refs, in_col, w_in):
    ch, cols = in_col.shape
    in_col[...] = jnp.transpose(jnp.broadcast_to(in_ref[...].astype(F32), (cols, ch)), (1, 0))
    for k, ref in enumerate(w_refs):
        w_in[k * ref.shape[1]:(k + 1) * ref.shape[1], :] = transposed(ref)


def merge_lanes(dst, at, blocks, cores):
    pieces = [jnp.transpose(b.astype(F32), (1, 0, 2)) for b in blocks]
    part = pieces[0].shape[2] // cores
    order = [p[:, :, r * part:(r + 1) * part] for r in range(cores) for p in pieces]
    dst[:, at:at + 8, :] = jnp.concatenate(order, axis=2)


def finish_row(row, summed, scale, w_gate, w_out):
    normed = normalise_row(row, scale)
    gate = jax.nn.sigmoid(jnp.dot(w_gate, normed, preferred_element_type=F32))
    update = jnp.dot(w_out, summed.astype(BF16), preferred_element_type=F32)
    return (row.astype(F32) + gate * update).astype(BF16)


def finish_kernel(cores, z_ref, n_ref, in_ref, w_gate_ref, w_out_ref, o_ref, sn, w_fin, in_col):
    rows, ch, cols = z_ref.shape
    steps, hid, _, lanes = n_ref.shape

    @pl.when(pl.program_id(0) == 0)
    def _():
        store_weights(in_ref, (w_gate_ref, w_out_ref), in_col, w_fin)

    for e in range(0, hid, 8):
        merge_lanes(sn, e, [n_ref[s, e:e + 8] for s in range(steps)], cores)

    def one_row(i, carry):
        o_ref[i] = finish_row(z_ref[i], sn[i], in_col[...], w_fin[:ch], w_fin[ch:])
        return carry

    lax.fori_loop(0, rows, one_row, 0, unroll=min(4, rows))


def finish(z_t, n_all, which, cores, in_row, w_gate, w_out):
    rows, ch, cols = z_t.shape
    hid, lanes = n_all.shape[1], n_all.shape[3]
    chunk = min(ROWS, rows)
    return pl.pallas_call(
        functools.partial(finish_kernel, cores),
        grid=(rows // chunk,),
        in_specs=[
            pl.BlockSpec((chunk, ch, cols), lambda i: (i, 0, 0)),
            pl.BlockSpec((STEPS, hid, chunk, lanes), lambda i: (which, 0, i, 0)),
            pl.BlockSpec((1, ch), lambda i: (0, 0)),
            pl.BlockSpec((ch, ch), lambda i: (0, 0)),
            pl.BlockSpec((hid, ch), lambda i: (0, 0)),
        ],
        out_specs=pl.BlockSpec((chunk, ch, cols), lambda i: (i, 0, 0)),
        out_shape=jax.ShapeDtypeStruct((rows, ch, cols), BF16),
        scratch_shapes=[pltpu.VMEM((chunk, hid, cols), F32), pltpu.VMEM((2 * ch, ch), BF16), pltpu.VMEM((ch, cols), F32)],
        name="finish",
    )(z_t, n_all, in_row, w_gate, w_out)


def exchange_kernel(ny, nx, cores, z0, z1, mask0, mask1, in_ref, wag_ref, wa_ref, wbg_ref, wb_ref, wg_ref, wo_ref, scale_ref,
                    out0, n_out, a_all, a_relay, by, b_relay, bx, bo, n_relay, a_in, b_in,
                    a_v, b_v, o_v, ssum, st, st_rx, st_in, mr, mr_in, nv, zbuf, sa, sb, obuf, nbuf, fbuf, w_in, w_fin, in_col,
                    send_sems, recv_sems, loc_sems):
    crops = 2
    z_in, mask_in = (z0, z1), (mask0, mask1)
    cb, rows, lanes = o_v.shape[2:]
    cols = a_v.shape[3]
    sub = lanes // cores
    hid = cb * ny
    half = cb // 2
    hr = rows // 2
    group = zbuf.shape[1]
    groups = rows // group
    per_step = groups // STEPS
    chunk = sa.shape[0]
    y = lax.axis_index("col")
    row_id = lax.axis_index("row")
    x, r = row_id // cores, row_id % cores
    yy = [lax.rem(y + d, ny) for d in range(ny)]
    to_y = [{"col": yy[d]} for d in range(ny)]
    both_y = ((0, to_y[1]), (1, to_y[3]))
    to_x = [{"row": lax.rem(x + e, nx) * cores + r} for e in range(nx)]
    to_p = {"row": x * cores + (cores - 1 - r)}
    e_of = [lax.rem(y + d + nx - x, nx) for d in range(ny)]

    counts = {"send": 0, "local": 0}
    sent = []

    def local(src, dst):
        k = counts["local"]
        counts["local"] += 1
        copy = pltpu.make_async_copy(src, dst, loc_sems.at[k])
        copy.start()
        return copy

    def load_z(g):
        t, h = divmod(g, groups)
        return local(z_in[t].at[pl.ds(h * group, group)], zbuf.at[g % 2])

    z_copy = {0: load_z(0)}

    barrier = pltpu.get_barrier_semaphore()
    peers = [to_y[1], to_y[3], to_x[1], to_x[3], to_p]
    for dev in peers:
        pl.semaphore_signal(barrier, inc=1, device_id=dev, device_id_type=MESH)
    pl.semaphore_wait(barrier, len(peers))

    def send(src, dst, dev):
        k = counts["send"]
        counts["send"] += 1
        copy = pltpu.make_async_remote_copy(
            src_ref=src, dst_ref=dst, send_sem=send_sems.at[k], recv_sem=recv_sems.at[k],
            device_id=dev, device_id_type=MESH)
        copy.start()
        sent.append(copy)
        return copy

    msg = {}
    early = (0, 1, 3)
    turns = {}

    def turn(*key):
        turns[key] = turns.get(key, -1) + 1
        return turns[key]

    stored = {}
    store_weights(in_ref, (wag_ref, wa_ref, wbg_ref, wb_ref), in_col, w_in)
    for k, ref in enumerate((wg_ref, wo_ref)):
        w_fin[k] = transposed(ref)

    def wait_stored(g):
        for copy in stored.pop(g, ()):
            copy.wait()

    def op_proj():
        g = turn("proj")
        t, h = divmod(g, groups)
        z_copy[g].wait()
        if g + 1 < crops * groups:
            z_copy[g + 1] = load_z(g + 1)
        wait_stored(g - 2)
        slot = g % 2

        def one_chunk(k, carry):
            def one_row(i, inner):
                row = k * chunk + i
                normed = normalise_row(zbuf[slot, row], in_col[...])
                prod = jnp.dot(w_in[...], normed, preferred_element_type=F32)
                mask = mask_in[t][pl.ds(h * group + row, 1), :].astype(F32)
                sa[i] = mask * jax.nn.sigmoid(prod[:hid]) * prod[hid:2 * hid]
                sb[i] = mask * jax.nn.sigmoid(prod[2 * hid:3 * hid]) * prod[3 * hid:]
                return inner

            lax.fori_loop(0, chunk, one_row, 0, unroll=min(4, chunk))
            place = pl.ds(pl.multiple_of(k * chunk, chunk), chunk)
            for e in range(0, hid, 8):
                obuf[slot, 0, e:e + 8, place, :] = jnp.transpose(sa[:, e:e + 8, :], (1, 0, 2)).astype(BF16)
                obuf[slot, 1, e:e + 8, place, :] = jnp.transpose(sb[:, e:e + 8, :], (1, 0, 2)).astype(BF16)
            return carry

        lax.fori_loop(0, group // chunk, one_chunk, 0)
        s, part = divmod(h, per_step)
        stored[g] = (
            local(obuf.at[slot, 0], a_in.at[t, :, pl.ds(h * group, group), :]),
            local(obuf.at[slot, 1], b_in.at[t, s, :, pl.ds(part * group, group), :]),
        )

    def a_piece(t, d):
        return a_in.at[t, pl.ds(yy[d] * cb, cb)]

    def b_piece(q, d):
        t, s = divmod(q, STEPS)
        return b_in.at[t, s, pl.ds(yy[d] * cb, cb)]

    def own_piece(q, e, d):
        if e == 0:
            return b_piece(q, 0) if d == 0 else by.at[q, d - 1]
        return bx.at[q, e - 1, d]

    def ready_rows(t, first, last):
        for h in range(first, last):
            wait_stored(t * groups + h)

    def op_a_relay(t):
        ready_rows(t, 0, groups)
        far = a_piece(t, 2)
        msg["ar", t, 0] = send(far.at[:half], a_relay.at[t, 0], to_y[1])
        msg["ar", t, 1] = send(far.at[half:], a_relay.at[t, 1], to_y[3])

    def op_a_dir(t):
        k = turn("a", t)
        part = pl.ds(k * half, half)
        msg["a", t, 3, k] = send(a_piece(t, 1).at[part], a_all.at[t, 2, part], to_y[1])
        msg["a", t, 1, k] = send(a_piece(t, 3).at[part], a_all.at[t, 0, part], to_y[3])

    def op_a_fwd(t):
        for k, dev in both_y:
            msg["ar", t, k].wait_recv()
            msg["a", t, 2, k] = send(a_relay.at[t, k], a_all.at[t, 1, pl.ds(k * half, half)], dev)

    def op_b_start(q):
        t, s = divmod(q, STEPS)
        ready_rows(t, s * per_step, (s + 1) * per_step)
        far = b_piece(q, 2)
        msg["br", q, 0] = send(far.at[:half], b_relay.at[q, 0], to_y[1])
        msg["br", q, 1] = send(far.at[half:], b_relay.at[q, 1], to_y[3])
        msg["b", q, 3] = send(b_piece(q, 1), by.at[q, 2], to_y[1])
        msg["b", q, 1] = send(b_piece(q, 3), by.at[q, 0], to_y[3])

    def op_b_fwd(q):
        for k, dev in both_y:
            msg["br", q, k].wait_recv()
            msg["bf", q, k] = send(b_relay.at[q, k], by.at[q, 1, pl.ds(k * half, half)], dev)

    def cross(q, e, d):
        msg["c", q, e, d] = send(own_piece(q, e, d), bo.at[q, e, d], to_p)

    def op_bx(q):
        d = (*early, 2)[turn("bx", q)]
        t, s = divmod(q, STEPS)
        if d == 0:
            ready_rows(t, s * per_step, (s + 1) * per_step)
        elif d == 2:
            msg["bf", q, 0].wait_recv()
            msg["bf", q, 1].wait_recv()
        else:
            msg["b", q, d].wait_recv()
        msg["x", q, 3, d] = send(own_piece(q, 0, d), bx.at[q, 2, d], to_x[1])
        msg["x", q, 1, d] = send(own_piece(q, 0, d), bx.at[q, 0, d], to_x[3])
        cross(q, 0, d)

    def op_xfwd(q):
        d = (*early, 2)[turn("xfwd", q)]
        for k, e in enumerate((3, 1)):
            part = pl.ds(k * half, half)
            msg["x", q, e, d].wait_recv()
            msg["xf", q, d, k] = send(bx.at[q, e - 1, d, part], bx.at[q, 1, d, part], to_x[4 - e])
        for e in (3, 1):
            cross(q, e, d)

    def op_xfar(q):
        d = (*early, 2)[turn("xfar", q)]
        msg["xf", q, d, 0].wait_recv()
        msg["xf", q, d, 1].wait_recv()
        cross(q, 2, d)

    loads = {}

    def load_b(q, ks):
        copies = []
        for d in ks:
            for e in range(nx):
                dst = pl.ds(pl.multiple_of(e * lanes + r * sub, sub), sub)
                copies.append(local(own_piece(q, e, d), b_v.at[d, :, dst, :]))
        for d in ks:
            for e in (0, 1, 3, 2):
                msg["c", q, e, d].wait_recv()
                dst = pl.ds(pl.multiple_of(e * lanes + (cores - 1 - r) * sub, sub), sub)
                copies.append(local(bo.at[q, e, d], b_v.at[d, :, dst, :]))
        return copies

    def op_load(q):
        loads["b", q] = load_b(q, early)

    def op_load2(q):
        loads["b2", q] = load_b(q, (2,))

    def op_load_a(t):
        copies = [local(a_piece(t, 0), a_v.at[0])]
        for d in (1, 3, 2):
            msg["a", t, d, 0].wait_recv()
            msg["a", t, d, 1].wait_recv()
            copies.append(local(a_all.at[t, d - 1], a_v.at[d]))
        loads["a", t] = copies

    def product(c, ks):
        acc = None
        for d in ks:
            term = lax.dot_general(a_v[d, c], b_v[d, c], (((1,), (1,)), ((), ())), preferred_element_type=F32)
            acc = term if acc is None else acc + term
        return acc

    def op_con(q):
        if q % STEPS == 0:
            for copy in loads["a", q // STEPS]:
                copy.wait()
        for copy in loads["b", q]:
            copy.wait()
        slot = q % 2

        def channel(c, carry):
            acc = product(c, early)
            for e in range(nx):
                o_v[slot, e, c] = acc[:, e * lanes:(e + 1) * lanes]
            return carry

        lax.fori_loop(0, cb, channel, 0)

    def op_con2(q):
        for copy in loads["b2", q]:
            copy.wait()
        slot = q % 2
        ssum[...] = jnp.zeros_like(ssum)

        def channel(c, carry):
            acc = product(c, (2,))
            for e in range(nx):
                part = o_v[slot, e, c] + acc[:, e * lanes:(e + 1) * lanes]
                o_v[slot, e, c] = part
                ssum[e] += part
            return carry

        lax.fori_loop(0, cb, channel, 0)
        block = min(16, hr)

        def squares(k, carry, h):
            rs = pl.ds(pl.multiple_of(h * hr + k * block, block), block)
            rh = pl.ds(pl.multiple_of(k * block, block), block)
            for e in range(nx):
                total = ssum[e, rs, :]
                mean = total * (1.0 / cb)
                acc = jnp.zeros_like(mean)
                for c in range(cb):
                    diff = o_v[slot, e, c, rs, :] - mean
                    acc = acc + diff * diff
                st[q, e, h, 0, rh, :] = total
                st[q, e, h, 1, rh, :] = acc
            return carry

        for h in range(2):
            lax.fori_loop(0, hr // block, functools.partial(squares, h=h), 0)
        msg["s", q, 0] = send(st.at[q, e_of[2], 0], st_rx.at[q, 0], to_y[1])
        msg["s", q, 1] = send(st.at[q, e_of[2], 1], st_rx.at[q, 1], to_y[3])

    def op_rs2(q):
        for k, d in ((0, 1), (1, 3)):
            msg["s", q, k].wait_recv()
            e = e_of[d]
            got_sum, got_sq = st_rx[q, k, 0], st_rx[q, k, 1]
            my_sum, my_sq = st[q, e, k, 0], st[q, e, k, 1]
            diff = (my_sum - got_sum) * (1.0 / cb)
            st[q, e, k, 0] = my_sum + got_sum
            st[q, e, k, 1] = my_sq + got_sq + (0.5 * cb) * (diff * diff)
            msg["t", q, k] = send(st.at[q, e], st_in.at[q, k], to_y[d])

    def op_red(q):
        msg["t", q, 0].wait_recv()
        msg["t", q, 1].wait_recv()
        for h in range(2):
            parts = [(st[q, e_of[0], h, 0], st[q, e_of[0], h, 1], cb)]
            for k in range(2):
                parts.append((st_in[q, k, h, 0], st_in[q, k, h, 1], 2 * cb if k == h else cb))
            mean = (parts[0][0] + parts[1][0] + parts[2][0]) * (1.0 / hid)
            m2 = jnp.zeros_like(mean)
            for total, sq, n in parts:
                diff = total * (1.0 / n) - mean
                m2 = m2 + sq + n * (diff * diff)
            mr[q, h, 0] = mean
            mr[q, h, 1] = lax.rsqrt(m2 * (1.0 / hid) + EPS)
        msg["m", q, 2] = send(mr.at[q], mr_in.at[q, 2], to_y[1])
        msg["m", q, 0] = send(mr.at[q], mr_in.at[q, 0], to_y[3])

    def apply_norm(q, d):
        e = e_of[d]
        for h in range(2):
            src = mr.at[q, h] if d == 0 else mr_in.at[q, d - 1, h]
            mean, rstd = src[0], src[1]

            def channel(c, carry, mean=mean, rstd=rstd, h=h):
                value = (o_v[q % 2, e, c, pl.ds(h * hr, hr), :] - mean) * rstd * scale_ref[y * cb + c]
                nv[q, d, c, pl.ds(h * hr, hr), :] = value.astype(BF16)
                return carry

            lax.fori_loop(0, cb, channel, 0)

    keep = {}

    def op_ag2(q):
        msg["m", q, 2].wait_recv()
        msg["mf", q, 0] = send(mr_in.at[q, 2, 0], mr_in.at[q, 1, 0], to_y[1])
        msg["m", q, 0].wait_recv()
        msg["mf", q, 1] = send(mr_in.at[q, 0, 1], mr_in.at[q, 1, 1], to_y[3])
        for d in (1, 3, 0):
            apply_norm(q, d)
        msg["n", q, 3] = send(nv.at[q, 1], n_out.at[q, y], to_y[1])
        msg["n", q, 1] = send(nv.at[q, 3], n_out.at[q, y], to_y[3])
        keep[q] = local(nv.at[q, 0], n_out.at[q, y])

    def op_norm(q):
        msg["mf", q, 0].wait_recv()
        msg["mf", q, 1].wait_recv()
        apply_norm(q, 2)
        msg["nr", q, 0] = send(nv.at[q, 2, pl.ds(0, half)], n_relay.at[q, 0], to_y[1])
        msg["nr", q, 1] = send(nv.at[q, 2, pl.ds(half, half)], n_relay.at[q, 1], to_y[3])

    def op_nfwd(q):
        for k, dev in both_y:
            msg["nr", q, k].wait_recv()
            owner = yy[3] if k == 0 else yy[1]
            msg["nf", q, k] = send(n_relay.at[q, k], n_out.at[q, owner, pl.ds(k * half, half)], dev)

    def op_nwait(q):
        for key in (("n", q, 1), ("n", q, 3), ("nf", q, 0), ("nf", q, 1)):
            msg[key].wait_recv()
        keep[q].wait()

    def op_fin():
        h = turn("fin")
        place = pl.ds(h * group, group)
        wait_stored(crops * groups - 2)
        wait_stored(crops * groups - 1)
        copies = [local(z0.at[place], zbuf.at[0])]
        for s in range(STEPS):
            copies.append(local(n_out.at[s, :, :, place, :], nbuf.at[s]))
        for copy in copies:
            copy.wait()
        if h:
            keep["f"].wait()

        def one_chunk(k, carry):
            at = pl.ds(pl.multiple_of(k * chunk, chunk), chunk)
            for blk in range(ny):
                for e in range(0, cb, 8):
                    merge_lanes(sa, blk * cb + e, [nbuf[s, blk, e:e + 8, at, :] for s in range(STEPS)], cores)

            def one_row(i, inner):
                row = k * chunk + i
                fbuf[row] = finish_row(zbuf[0, row], sa[i], in_col[...], w_fin[0], w_fin[1])
                return inner

            lax.fori_loop(0, chunk, one_row, 0, unroll=min(4, chunk))
            return carry

        lax.fori_loop(0, group // chunk, one_chunk, 0)
        keep["f"] = local(fbuf, out0.at[place])

    table = dict(proj=op_proj, a_relay=op_a_relay, a_dir=op_a_dir, a_fwd=op_a_fwd, b_start=op_b_start, b_fwd=op_b_fwd,
                 bx=op_bx, xfwd=op_xfwd, xfar=op_xfar, load=op_load, load_a=op_load_a, load2=op_load2, con=op_con, con2=op_con2, rs2=op_rs2,
                 red=op_red, ag2=op_ag2, norm=op_norm, nfwd=op_nfwd, nwait=op_nwait, fin=op_fin)
    for name, *where in ORDER:
        with jax.named_scope("_".join([name, *map(str, where)])):
            table[name](*where)
    keep["f"].wait()
    for copy in sent:
        copy.wait_send()


def exchange(crops, masks, in_row, weights, scale, ny, nx, cores):
    rows, ch, cols = crops[0].shape
    hid = scale.shape[0]
    cb = hid // ny
    sub = rows // STEPS
    lanes = cores * sub
    hr = rows // 2
    q = 2 * STEPS
    group = rows // 4
    chunk = min(ROWS, group)
    any_spec = pl.BlockSpec(memory_space=pl.ANY)
    vmem = pl.BlockSpec(memory_space=pltpu.VMEM)

    def hbm(*shape):
        return jax.ShapeDtypeStruct(shape, BF16)

    sends = 2 * 8 + q * (6 + 4 * ny + nx * ny + 8 + 6)
    locals_ = 8 + 16 + q * (2 * nx * ny) + 2 * ny + q + 4 * (2 + STEPS)
    outs = pl.pallas_call(
        functools.partial(exchange_kernel, ny, nx, cores),
        in_specs=[any_spec] * 2 + [vmem] * (3 + len(weights)) + [pl.BlockSpec(memory_space=pltpu.SMEM)],
        out_specs=[any_spec] * 11,
        out_shape=[
            hbm(rows, ch, cols),
            hbm(q, ny, cb, rows, lanes),
            hbm(2, ny - 1, cb, rows, cols),
            hbm(2, 2, cb // 2, rows, cols),
            hbm(q, ny - 1, cb, sub, cols),
            hbm(q, 2, cb // 2, sub, cols),
            hbm(q, nx - 1, ny, cb, sub, cols),
            hbm(q, nx, ny, cb, sub, cols),
            hbm(q, 2, cb // 2, rows, lanes),
            hbm(2, hid, rows, cols),
            hbm(2, STEPS, hid, sub, cols),
        ],
        scratch_shapes=[
            pltpu.VMEM((ny, cb, rows, cols), BF16),
            pltpu.VMEM((ny, cb, nx * lanes, cols), BF16),
            pltpu.VMEM((2, nx, cb, rows, lanes), F32),
            pltpu.VMEM((nx, rows, lanes), F32),
            pltpu.VMEM((q, nx, 2, 2, hr, lanes), F32),
            pltpu.VMEM((q, 2, 2, hr, lanes), F32),
            pltpu.VMEM((q, 2, 2, 2, hr, lanes), F32),
            pltpu.VMEM((q, 2, 2, hr, lanes), F32),
            pltpu.VMEM((q, ny - 1, 2, 2, hr, lanes), F32),
            pltpu.VMEM((q, ny, cb, rows, lanes), BF16),
            pltpu.VMEM((2, group, ch, cols), BF16),
            pltpu.VMEM((chunk, hid, cols), F32),
            pltpu.VMEM((chunk, hid, cols), F32),
            pltpu.VMEM((2, 2, hid, group, cols), BF16),
            pltpu.VMEM((STEPS, ny, cb, group, lanes), BF16),
            pltpu.VMEM((group, ch, cols), BF16),
            pltpu.VMEM((4 * hid, ch), BF16),
            pltpu.VMEM((2, ch, hid), BF16),
            pltpu.VMEM((ch, cols), F32),
            pltpu.SemaphoreType.DMA((sends,)),
            pltpu.SemaphoreType.DMA((sends,)),
            pltpu.SemaphoreType.DMA((locals_,)),
        ],
        compiler_params=pltpu.CompilerParams(collective_id=0, has_side_effects=True, vmem_limit_bytes=VMEM_LIMIT),
        cost_estimate=pl.CostEstimate(flops=4 * rows * cols * hid * nx * cols, bytes_accessed=200000000, transcendentals=0),
        name="exchange",
    )(*crops, *masks, in_row, *weights, scale)
    return outs[0], outs[1].reshape(q, hid, rows, lanes)


def solution(mesh):
    row_count = mesh.shape['row']
    col_count = mesh.shape['col']
    cores = row_count // col_count
    nx = row_count // cores
    pair_spec = P(('batch', 'row'), 'col', None)
    mask_spec = P(('batch', 'row'), 'col')
    replicated = P()

    def device_fn(z_one, z_two, mask_one, mask_two, ln_in_scale, w_a, w_a_gate, w_b, w_b_gate, w_gate, w_out, ln_out_scale):
        in_row = ln_in_scale[None, :]
        crops = [jnp.transpose(z, (0, 2, 1)) for z in (z_one, z_two)]
        first, n_all = exchange(crops, (mask_one, mask_two), in_row, (w_a_gate, w_a, w_b_gate, w_b, w_gate, w_out),
                                ln_out_scale.astype(F32), col_count, nx, cores)
        second = finish(crops[1], n_all, 1, cores, in_row, w_gate, w_out)
        return tuple(jnp.transpose(o, (0, 2, 1)) for o in (first, second))

    return jax.shard_map(
        device_fn,
        mesh=mesh,
        in_specs=(pair_spec, pair_spec, mask_spec, mask_spec) + (replicated,) * 8,
        out_specs=(pair_spec, pair_spec),
        check_vma=False,
    )
```

```python
import functools
import jax
import jax.numpy as jnp
from jax import lax
from jax.experimental import pallas as pl
from jax.experimental.pallas import tpu as pltpu
from jax.sharding import PartitionSpec as P

MESH = pl.DeviceIdType.MESH
F32 = jnp.float32
BF16 = jnp.bfloat16
EPS = 1e-5
STEPS = 2
ROWS = 16
VMEM_LIMIT = 60 * 1024 * 1024
ORDER = (
    'proj', 'proj', 'bx', 'b_start', 'proj', 'proj', 'a_relay', 'b_fwd', 'xfwd', 'bx', 'bx', 'proj', 'proj', 'a_fwd', 'xfwd',
    'proj', 'xfar', 'bx', 'bx', 'b_start', 'bx', 'b_fwd', 'bx', 'a_dir', 'xfwd', 'xfwd', 'a_dir', 'proj', 'b_start', 'bx',
    'b_start', 'xfwd', 'xfwd', 'xfwd', 'load_a', 'bx', 'bx', 'xfar', 'xfar', 'xfar', 'a_relay', 'xfar', 'load', 'con', 'bx',
    'load2', 'con2', 'a_dir', 'xfwd', 'xfar', 'xfar', 'load', 'b_fwd', 'b_fwd', 'xfwd', 'a_dir', 'xfar', 'xfwd', 'a_fwd', 'rs2',
    'con2', 'load2', 'bx', 'con', 'xfar', 'xfar', 'con2', 'red', 'rs2', 'ag2', 'xfwd', 'red', 'xfwd', 'con2', 'norm', 'xfar',
    'ag2', 'load', 'rs2', 'bx', 'bx', 'bx', 'xfar', 'load2', 'red', 'ag2', 'norm', 'norm', 'nfwd', 'load_a', 'con', 'con2',
    'rs2', 'nfwd', 'con2', 'rs2', 'red', 'xfwd', 'xfwd', 'rs2', 'xfwd', 'nfwd', 'red', 'red', 'bx', 'xfar', 'ag2', 'nwait',
    'nwait', 'nwait', 'fin', 'ag2', 'norm', 'ag2', 'xfar', 'xfar', 'load', 'fin', 'norm', 'norm', 'xfwd', 'con', 'nfwd', 'nfwd',
    'xfar', 'load2', 'nwait', 'nfwd', 'con2', 'rs2', 'con2', 'nwait', 'nwait', 'red', 'rs2', 'ag2', 'norm', 'red', 'fin', 'nfwd',
    'ag2', 'fin', 'norm', 'nwait', 'fin', 'nfwd', 'fin', 'nwait',
)


def normalise_row(row, scale):
    values = row.astype(F32)
    count = values.shape[0]
    mean = jnp.sum(values, axis=0, keepdims=True) / count
    centered = values - mean
    variance = jnp.sum(centered * centered, axis=0, keepdims=True) / count
    return (centered * lax.rsqrt(variance + EPS) * scale).astype(BF16)


def transposed(ref):
    return jnp.transpose(ref[...].astype(F32), (1, 0)).astype(BF16)


def store_weights(in_ref, w_refs, in_col, w_in):
    ch, cols = in_col.shape
    in_col[...] = jnp.transpose(jnp.broadcast_to(in_ref[...].astype(F32), (cols, ch)), (1, 0))
    for k, ref in enumerate(w_refs):
        w_in[k * ref.shape[1]:(k + 1) * ref.shape[1], :] = transposed(ref)


def merge_lanes(dst, at, blocks, cores):
    pieces = [jnp.transpose(b.astype(F32), (1, 0, 2)) for b in blocks]
    part = pieces[0].shape[2] // cores
    order = [p[:, :, r * part:(r + 1) * part] for r in range(cores) for p in pieces]
    dst[:, at:at + 8, :] = jnp.concatenate(order, axis=2)


def finish_row(row, summed, scale, w_gate, w_out):
    normed = normalise_row(row, scale)
    gate = jax.nn.sigmoid(jnp.dot(w_gate, normed, preferred_element_type=F32))
    update = jnp.dot(w_out, summed.astype(BF16), preferred_element_type=F32)
    return (row.astype(F32) + gate * update).astype(BF16)


def finish_kernel(cores, done_one, done_two, z_ref, n_ref, in_ref, w_gate_ref, w_out_ref, one_ref, two_ref, sn, w_fin, in_col):
    rows, ch, cols = z_ref.shape
    steps, hid, _, lanes = n_ref.shape

    @pl.when(pl.program_id(0) == 0)
    def _():
        store_weights(in_ref, (w_gate_ref, w_out_ref), in_col, w_fin)

    one_ref[...] = done_one[...]
    two_ref[0] = done_two[...]
    for e in range(0, hid, 8):
        merge_lanes(sn, e, [n_ref[s, e:e + 8] for s in range(steps)], cores)

    def one_row(i, carry):
        two_ref[1, i] = finish_row(z_ref[i], sn[i], in_col[...], w_fin[:ch], w_fin[ch:])
        return carry

    lax.fori_loop(0, rows, one_row, 0, unroll=min(4, rows))


def finish(z_t, done, n_all, cores, in_row, w_gate, w_out):
    rows, ch, cols = z_t.shape
    hid, lanes = n_all.shape[1], n_all.shape[3]
    hp = rows // 2
    chunk = min(ROWS, hp)
    steps = hp // chunk
    one, two = pl.pallas_call(
        functools.partial(finish_kernel, cores),
        grid=(steps,),
        in_specs=[
            pl.BlockSpec((2 * chunk, ch, cols), lambda i: (i, 0, 0)),
            pl.BlockSpec((chunk, ch, cols), lambda i: (2 * steps + i, 0, 0)),
            pl.BlockSpec((chunk, ch, cols), lambda i: (steps + i, 0, 0)),
            pl.BlockSpec((STEPS, hid, chunk, lanes), lambda i: (1, 0, steps + i, 0)),
            pl.BlockSpec((1, ch), lambda i: (0, 0)),
            pl.BlockSpec((ch, ch), lambda i: (0, 0)),
            pl.BlockSpec((hid, ch), lambda i: (0, 0)),
        ],
        out_specs=[
            pl.BlockSpec((2 * chunk, ch, cols), lambda i: (i, 0, 0)),
            pl.BlockSpec((2, chunk, ch, cols), lambda i: (0, i, 0, 0)),
        ],
        out_shape=[jax.ShapeDtypeStruct((rows, ch, cols), BF16), jax.ShapeDtypeStruct((2, hp, ch, cols), BF16)],
        scratch_shapes=[pltpu.VMEM((chunk, hid, cols), F32), pltpu.VMEM((2 * ch, ch), BF16), pltpu.VMEM((ch, cols), F32)],
        name="finish",
    )(done, done, z_t, n_all, in_row, w_gate, w_out)
    return one, two.reshape(rows, ch, cols)


def exchange_kernel(ny, nx, cores, z0, z1, mask0, mask1, in_ref, wag_ref, wa_ref, wbg_ref, wb_ref, wg_ref, wo_ref, out_ref,
                    done, n_out, a_all, a_relay, by, b_relay, bx, bo, n_relay, a_in, b_in,
                    a_v, b_v, o_v, ssum, st, st_rx, st_in, mr, mr_in, nv, zbuf, sa, sb, obuf, nbuf, fbuf, w_in, w_fin, in_col, out_col,
                    send_sems, recv_sems, loc_sems):
    crops = 2
    z_in, mask_in = (z0, z1), (mask0, mask1)
    cb, rows, lanes = o_v.shape[2:]
    cols = a_v.shape[3]
    sub = lanes // cores
    hid = cb * ny
    half = cb // 2
    hp = rows // 2
    hr = hp // 2
    group = zbuf.shape[1]
    groups = rows // group
    per_step = groups // STEPS
    chunk = sa.shape[0]
    y = lax.axis_index("col")
    row_id = lax.axis_index("row")
    x, r = row_id // cores, row_id % cores
    yy = [lax.rem(y + d, ny) for d in range(ny)]
    to_y = [{"col": yy[d]} for d in range(ny)]
    both_y = ((0, to_y[1]), (1, to_y[3]))
    to_x = [{"row": lax.rem(x + e, nx) * cores + r} for e in range(nx)]
    to_p = {"row": x * cores + (cores - 1 - r)}
    e_of = [lax.rem(y + d + nx - x, nx) for d in range(ny)]

    counts = {"send": 0, "local": 0}
    sent = []

    def local(src, dst):
        k = counts["local"]
        counts["local"] += 1
        copy = pltpu.make_async_copy(src, dst, loc_sems.at[k])
        copy.start()
        return copy

    def load_z(g):
        t, h = divmod(g, groups)
        return local(z_in[t].at[pl.ds(h * group, group)], zbuf.at[g % 2])

    barrier = pltpu.get_barrier_semaphore()
    peers = [to_y[1], to_y[3], to_x[1], to_x[3], to_p]
    for dev in peers:
        pl.semaphore_signal(barrier, inc=1, device_id=dev, device_id_type=MESH)
    def send(src, dst, dev):
        k = counts["send"]
        if k == 0:
            pl.semaphore_wait(barrier, len(peers))
        counts["send"] += 1
        copy = pltpu.make_async_remote_copy(
            src_ref=src, dst_ref=dst, send_sem=send_sems.at[k], recv_sem=recv_sems.at[k],
            device_id=dev, device_id_type=MESH)
        copy.start()
        sent.append(copy)
        return copy

    z_copy = {0: load_z(0)}
    msg = {}
    early = (0, 1, 3)
    turns = {}

    def turn(*key):
        turns[key] = turns.get(key, -1) + 1
        return turns[key]

    def x_turn(name):
        q, k = divmod(turn(name), ny)
        return q, (*early, 2)[k]

    stored = {}
    store_weights(in_ref, (wag_ref, wa_ref, wbg_ref, wb_ref), in_col, w_in)
    for k, ref in enumerate((wg_ref, wo_ref)):
        w_fin[k] = transposed(ref)
    out_col[...] = jnp.transpose(jnp.broadcast_to(out_ref[...].astype(F32), (lanes, hid)), (1, 0))

    def wait_stored(g):
        for copy in stored.pop(g, ()):
            copy.wait()

    def op_proj():
        g = turn("proj")
        t, h = divmod(g, groups)
        z_copy[g].wait()
        if g + 1 < crops * groups:
            z_copy[g + 1] = load_z(g + 1)
        wait_stored(g - 2)
        slot = g % 2

        def one_chunk(k, carry):
            def one_row(i, inner):
                row = k * chunk + i
                normed = normalise_row(zbuf[slot, row], in_col[...])
                prod = jnp.dot(w_in[...], normed, preferred_element_type=F32)
                mask = mask_in[t][pl.ds(h * group + row, 1), :].astype(F32)
                sa[i] = mask * jax.nn.sigmoid(prod[:hid]) * prod[hid:2 * hid]
                sb[i] = mask * jax.nn.sigmoid(prod[2 * hid:3 * hid]) * prod[3 * hid:]
                return inner

            lax.fori_loop(0, chunk, one_row, 0, unroll=min(4, chunk))
            place = pl.ds(pl.multiple_of(k * chunk, chunk), chunk)
            for e in range(0, hid, 8):
                obuf[slot, 0, e:e + 8, place, :] = jnp.transpose(sa[:, e:e + 8, :], (1, 0, 2)).astype(BF16)
                obuf[slot, 1, e:e + 8, place, :] = jnp.transpose(sb[:, e:e + 8, :], (1, 0, 2)).astype(BF16)
            return carry

        lax.fori_loop(0, group // chunk, one_chunk, 0)
        s, part = divmod(h, per_step)
        stored[g] = (
            local(obuf.at[slot, 0], a_in.at[t, :, pl.ds(h * group, group), :]),
            local(obuf.at[slot, 1], b_in.at[t, s, :, pl.ds(part * group, group), :]),
        )

    def a_piece(t, d):
        return a_in.at[t, pl.ds(yy[d] * cb, cb)]

    def b_piece(q, d):
        t, s = divmod(q, STEPS)
        return b_in.at[t, s, pl.ds(yy[d] * cb, cb)]

    def own_piece(q, e, d):
        if e == 0:
            return b_piece(q, 0) if d == 0 else by.at[q, d - 1]
        return bx.at[q, e - 1, d]

    def ready_rows(t, first, last):
        for h in range(first, last):
            wait_stored(t * groups + h)

    def op_a_relay():
        t = turn("a_relay")
        ready_rows(t, 0, groups)
        far = a_piece(t, 2)
        msg["ar", t, 0] = send(far.at[:half], a_relay.at[t, 0], to_y[1])
        msg["ar", t, 1] = send(far.at[half:], a_relay.at[t, 1], to_y[3])

    def op_a_dir():
        t, k = divmod(turn("a_dir"), 2)
        part = pl.ds(k * half, half)
        msg["a", t, 3, k] = send(a_piece(t, 1).at[part], a_all.at[t, 2, part], to_y[1])
        msg["a", t, 1, k] = send(a_piece(t, 3).at[part], a_all.at[t, 0, part], to_y[3])

    def op_a_fwd():
        t = turn("a_fwd")
        for k, dev in both_y:
            msg["ar", t, k].wait_recv()
            msg["a", t, 2, k] = send(a_relay.at[t, k], a_all.at[t, 1, pl.ds(k * half, half)], dev)

    def op_b_start():
        q = turn("b_start")
        t, s = divmod(q, STEPS)
        ready_rows(t, s * per_step, (s + 1) * per_step)
        far = b_piece(q, 2)
        msg["br", q, 0] = send(far.at[:half], b_relay.at[q, 0], to_y[1])
        msg["br", q, 1] = send(far.at[half:], b_relay.at[q, 1], to_y[3])
        msg["b", q, 3] = send(b_piece(q, 1), by.at[q, 2], to_y[1])
        msg["b", q, 1] = send(b_piece(q, 3), by.at[q, 0], to_y[3])

    def op_b_fwd():
        q = turn("b_fwd")
        for k, dev in both_y:
            msg["br", q, k].wait_recv()
            msg["bf", q, k] = send(b_relay.at[q, k], by.at[q, 1, pl.ds(k * half, half)], dev)

    def cross(q, e, d):
        msg["c", q, e, d] = send(own_piece(q, e, d), bo.at[q, e, d], to_p)

    def op_bx():
        q, d = x_turn("bx")
        t, s = divmod(q, STEPS)
        if d == 0:
            ready_rows(t, s * per_step, (s + 1) * per_step)
        elif d == 2:
            msg["bf", q, 0].wait_recv()
            msg["bf", q, 1].wait_recv()
        else:
            msg["b", q, d].wait_recv()
        msg["x", q, 3, d] = send(own_piece(q, 0, d), bx.at[q, 2, d], to_x[1])
        msg["x", q, 1, d] = send(own_piece(q, 0, d), bx.at[q, 0, d], to_x[3])
        cross(q, 0, d)

    def op_xfwd():
        q, d = x_turn("xfwd")
        for k, e in enumerate((3, 1)):
            part = pl.ds(k * half, half)
            msg["x", q, e, d].wait_recv()
            msg["xf", q, d, k] = send(bx.at[q, e - 1, d, part], bx.at[q, 1, d, part], to_x[4 - e])
        for e in (3, 1):
            cross(q, e, d)

    def op_xfar():
        q, d = x_turn("xfar")
        msg["xf", q, d, 0].wait_recv()
        msg["xf", q, d, 1].wait_recv()
        cross(q, 2, d)

    loads = {}

    def load_b(q, ks):
        copies = []
        for d in ks:
            for e in range(nx):
                dst = pl.ds(pl.multiple_of(e * lanes + r * sub, sub), sub)
                copies.append(local(own_piece(q, e, d), b_v.at[d, :, dst, :]))
        for d in ks:
            for e in (0, 1, 3, 2):
                msg["c", q, e, d].wait_recv()
                dst = pl.ds(pl.multiple_of(e * lanes + (cores - 1 - r) * sub, sub), sub)
                copies.append(local(bo.at[q, e, d], b_v.at[d, :, dst, :]))
        return copies

    def op_load():
        q = turn("load")
        loads["b", q] = load_b(q, early)

    def op_load2():
        q = turn("load2")
        loads["b2", q] = load_b(q, (2,))

    def op_load_a():
        t = turn("load_a")
        copies = [local(a_piece(t, 0), a_v.at[0])]
        for d in (1, 3, 2):
            msg["a", t, d, 0].wait_recv()
            msg["a", t, d, 1].wait_recv()
            copies.append(local(a_all.at[t, d - 1], a_v.at[d]))
        loads["a", t] = copies

    def product(c, ks, rs):
        acc = None
        for d in ks:
            term = lax.dot_general(a_v[d, c, rs, :], b_v[d, c], (((1,), (1,)), ((), ())), preferred_element_type=F32)
            acc = term if acc is None else acc + term
        return acc

    def op_con():
        q = turn("con")
        if q % STEPS == 0:
            for copy in loads["a", q // STEPS]:
                copy.wait()
        for copy in loads["b", q]:
            copy.wait()
        slot = q % 2

        def channel(c, carry):
            acc = product(c, early, pl.ds(0, rows))
            for e in range(nx):
                o_v[slot, e, c] = acc[:, e * lanes:(e + 1) * lanes]
            return carry

        lax.fori_loop(0, cb, channel, 0)

    def op_con2():
        u = turn("con2")
        q, p = divmod(u, 2)
        if p == 0:
            for copy in loads["b2", q]:
                copy.wait()
        slot = q % 2
        rp = pl.ds(p * hp, hp)
        ssum[...] = jnp.zeros_like(ssum)

        def channel(c, carry):
            acc = product(c, (2,), rp)
            for e in range(nx):
                part = o_v[slot, e, c, rp, :] + acc[:, e * lanes:(e + 1) * lanes]
                o_v[slot, e, c, rp, :] = part
                ssum[e] += part
            return carry

        lax.fori_loop(0, cb, channel, 0)
        block = min(16, hr)

        def squares(k, carry, h):
            rs = pl.ds(pl.multiple_of(h * hr + k * block, block), block)
            ro = pl.ds(pl.multiple_of(p * hp + h * hr + k * block, block), block)
            rh = pl.ds(pl.multiple_of(k * block, block), block)
            for e in range(nx):
                total = ssum[e, rs, :]
                mean = total * (1.0 / cb)
                acc = jnp.zeros_like(mean)
                for c in range(cb):
                    diff = o_v[slot, e, c, ro, :] - mean
                    acc = acc + diff * diff
                st[u, e, h, 0, rh, :] = total
                st[u, e, h, 1, rh, :] = acc
            return carry

        for h in range(2):
            lax.fori_loop(0, hr // block, functools.partial(squares, h=h), 0)
        msg["s", u, 0] = send(st.at[u, e_of[2], 0], st_rx.at[u, 0], to_y[1])
        msg["s", u, 1] = send(st.at[u, e_of[2], 1], st_rx.at[u, 1], to_y[3])

    def op_rs2():
        u = turn("rs2")
        for k, d in ((0, 1), (1, 3)):
            msg["s", u, k].wait_recv()
            e = e_of[d]
            got_sum, got_sq = st_rx[u, k, 0], st_rx[u, k, 1]
            my_sum, my_sq = st[u, e, k, 0], st[u, e, k, 1]
            diff = (my_sum - got_sum) * (1.0 / cb)
            st[u, e, k, 0] = my_sum + got_sum
            st[u, e, k, 1] = my_sq + got_sq + (0.5 * cb) * (diff * diff)
            msg["t", u, k] = send(st.at[u, e], st_in.at[u, k], to_y[d])

    def op_red():
        u = turn("red")
        msg["t", u, 0].wait_recv()
        msg["t", u, 1].wait_recv()
        for h in range(2):
            parts = [(st[u, e_of[0], h, 0], st[u, e_of[0], h, 1], cb)]
            for k in range(2):
                parts.append((st_in[u, k, h, 0], st_in[u, k, h, 1], 2 * cb if k == h else cb))
            mean = (parts[0][0] + parts[1][0] + parts[2][0]) * (1.0 / hid)
            m2 = jnp.zeros_like(mean)
            for total, sq, n in parts:
                diff = total * (1.0 / n) - mean
                m2 = m2 + sq + n * (diff * diff)
            mr[u, h, 0] = mean
            mr[u, h, 1] = lax.rsqrt(m2 * (1.0 / hid) + EPS)
        msg["m", u, 2] = send(mr.at[u], mr_in.at[u, 2], to_y[1])
        msg["m", u, 0] = send(mr.at[u], mr_in.at[u, 0], to_y[3])

    def apply_norm(u, d):
        q, p = divmod(u, 2)
        e = e_of[d]
        for h in range(2):
            src = mr.at[u, h] if d == 0 else mr_in.at[u, d - 1, h]
            mean, rstd = src[0], src[1]

            def channel(c, carry, mean=mean, rstd=rstd, h=h):
                scale = out_col[pl.ds(y * cb + c, 1), :]
                value = (o_v[q % 2, e, c, pl.ds(p * hp + h * hr, hr), :] - mean) * rstd * scale
                nv[u, d, c, pl.ds(h * hr, hr), :] = value.astype(BF16)
                return carry

            lax.fori_loop(0, cb, channel, 0)

    def n_place(u, owner, *part):
        q, p = divmod(u, 2)
        return n_out.at[q, owner, *(part or (slice(None),)), pl.ds(p * hp, hp), :]

    keep = {}

    def op_ag2():
        u = turn("ag2")
        msg["m", u, 2].wait_recv()
        msg["mf", u, 0] = send(mr_in.at[u, 2, 0], mr_in.at[u, 1, 0], to_y[1])
        msg["m", u, 0].wait_recv()
        msg["mf", u, 1] = send(mr_in.at[u, 0, 1], mr_in.at[u, 1, 1], to_y[3])
        for d in (1, 3, 0):
            apply_norm(u, d)
        msg["n", u, 3] = send(nv.at[u, 1], n_place(u, y), to_y[1])
        msg["n", u, 1] = send(nv.at[u, 3], n_place(u, y), to_y[3])
        keep[u] = local(nv.at[u, 0], n_place(u, y))

    def op_norm():
        u = turn("norm")
        msg["mf", u, 0].wait_recv()
        msg["mf", u, 1].wait_recv()
        apply_norm(u, 2)
        msg["nr", u, 0] = send(nv.at[u, 2, pl.ds(0, half)], n_relay.at[u, 0], to_y[1])
        msg["nr", u, 1] = send(nv.at[u, 2, pl.ds(half, half)], n_relay.at[u, 1], to_y[3])

    def op_nfwd():
        u = turn("nfwd")
        for k, dev in both_y:
            msg["nr", u, k].wait_recv()
            owner = yy[3] if k == 0 else yy[1]
            msg["nf", u, k] = send(n_relay.at[u, k], n_place(u, owner, pl.ds(k * half, half)), dev)

    def op_nwait():
        u = turn("nwait")
        for key in (("n", u, 1), ("n", u, 3), ("nf", u, 0), ("nf", u, 1)):
            msg[key].wait_recv()
        keep[u].wait()

    def op_fin():
        f = turn("fin")
        t, h = divmod(f, groups)
        place = pl.ds(h * group, group)
        wait_stored(crops * groups - 2)
        wait_stored(crops * groups - 1)
        copies = [local(z_in[t].at[place], zbuf.at[0])]
        for s in range(STEPS):
            copies.append(local(n_out.at[t * STEPS + s, :, :, place, :], nbuf.at[s]))
        for copy in copies:
            copy.wait()
        if f:
            keep["f"].wait()

        def one_chunk(k, carry):
            at = pl.ds(pl.multiple_of(k * chunk, chunk), chunk)
            for blk in range(ny):
                for e in range(0, cb, 8):
                    merge_lanes(sa, blk * cb + e, [nbuf[s, blk, e:e + 8, at, :] for s in range(STEPS)], cores)

            def one_row(i, inner):
                row = k * chunk + i
                fbuf[row] = finish_row(zbuf[0, row], sa[i], in_col[...], w_fin[0], w_fin[1])
                return inner

            lax.fori_loop(0, chunk, one_row, 0, unroll=min(4, chunk))
            return carry

        lax.fori_loop(0, group // chunk, one_chunk, 0)
        keep["f"] = local(fbuf, done.at[pl.ds(f * group, group)])

    table = dict(proj=op_proj, a_relay=op_a_relay, a_dir=op_a_dir, a_fwd=op_a_fwd, b_start=op_b_start, b_fwd=op_b_fwd,
                 bx=op_bx, xfwd=op_xfwd, xfar=op_xfar, load=op_load, load_a=op_load_a, load2=op_load2, con=op_con, con2=op_con2, rs2=op_rs2,
                 red=op_red, ag2=op_ag2, norm=op_norm, nfwd=op_nfwd, nwait=op_nwait, fin=op_fin)
    for name in ORDER:
        with jax.named_scope(name):
            table[name]()
    keep["f"].wait()
    for copy in sent:
        copy.wait_send()


def exchange(crops, masks, rows_in, ny, nx, cores):
    rows, ch, cols = crops[0].shape
    hid = rows_in[-1].shape[1]
    cb = hid // ny
    sub = rows // STEPS
    lanes = cores * sub
    hp = rows // 2
    hr = hp // 2
    q = 2 * STEPS
    u = 2 * q
    group = rows // 4
    chunk = min(ROWS, group)
    any_spec = pl.BlockSpec(memory_space=pl.ANY)
    vmem = pl.BlockSpec(memory_space=pltpu.VMEM)

    def hbm(*shape):
        return jax.ShapeDtypeStruct(shape, BF16)

    sends = 2 * 8 + q * (6 + 4 * ny + nx * ny) + u * (8 + 6)
    locals_ = 8 + 16 + q * (2 * nx * ny) + 2 * ny + u + 6 * (2 + STEPS)
    outs = pl.pallas_call(
        functools.partial(exchange_kernel, ny, nx, cores),
        in_specs=[any_spec] * 2 + [vmem] * (2 + len(rows_in)),
        out_specs=[any_spec] * 11,
        out_shape=[
            hbm(rows + hp, ch, cols),
            hbm(q, ny, cb, rows, lanes),
            hbm(2, ny - 1, cb, rows, cols),
            hbm(2, 2, cb // 2, rows, cols),
            hbm(q, ny - 1, cb, sub, cols),
            hbm(q, 2, cb // 2, sub, cols),
            hbm(q, nx - 1, ny, cb, sub, cols),
            hbm(q, nx, ny, cb, sub, cols),
            hbm(u, 2, cb // 2, hp, lanes),
            hbm(2, hid, rows, cols),
            hbm(2, STEPS, hid, sub, cols),
        ],
        scratch_shapes=[
            pltpu.VMEM((ny, cb, rows, cols), BF16),
            pltpu.VMEM((ny, cb, nx * lanes, cols), BF16),
            pltpu.VMEM((2, nx, cb, rows, lanes), F32),
            pltpu.VMEM((nx, hp, lanes), F32),
            pltpu.VMEM((u, nx, 2, 2, hr, lanes), F32),
            pltpu.VMEM((u, 2, 2, hr, lanes), F32),
            pltpu.VMEM((u, 2, 2, 2, hr, lanes), F32),
            pltpu.VMEM((u, 2, 2, hr, lanes), F32),
            pltpu.VMEM((u, ny - 1, 2, 2, hr, lanes), F32),
            pltpu.VMEM((u, ny, cb, hp, lanes), BF16),
            pltpu.VMEM((2, group, ch, cols), BF16),
            pltpu.VMEM((chunk, hid, cols), F32),
            pltpu.VMEM((chunk, hid, cols), F32),
            pltpu.VMEM((2, 2, hid, group, cols), BF16),
            pltpu.VMEM((STEPS, ny, cb, group, lanes), BF16),
            pltpu.VMEM((group, ch, cols), BF16),
            pltpu.VMEM((4 * hid, ch), BF16),
            pltpu.VMEM((2, ch, hid), BF16),
            pltpu.VMEM((ch, cols), F32),
            pltpu.VMEM((hid, lanes), F32),
            pltpu.SemaphoreType.DMA((sends,)),
            pltpu.SemaphoreType.DMA((sends,)),
            pltpu.SemaphoreType.DMA((locals_,)),
        ],
        compiler_params=pltpu.CompilerParams(collective_id=0, has_side_effects=True, vmem_limit_bytes=VMEM_LIMIT),
        cost_estimate=pl.CostEstimate(flops=4 * rows * cols * hid * nx * cols, bytes_accessed=200000000, transcendentals=0),
        name="exchange",
    )(*crops, *masks, *rows_in)
    return outs[0], outs[1].reshape(q, hid, rows, lanes)


def solution(mesh):
    row_count = mesh.shape['row']
    col_count = mesh.shape['col']
    cores = row_count // col_count
    nx = row_count // cores
    pair_spec = P(('batch', 'row'), 'col', None)
    mask_spec = P(('batch', 'row'), 'col')
    replicated = P()

    def device_fn(z_one, z_two, mask_one, mask_two, ln_in_scale, w_a, w_a_gate, w_b, w_b_gate, w_gate, w_out, ln_out_scale):
        in_row = ln_in_scale[None, :]
        crops = [jnp.transpose(z, (0, 2, 1)) for z in (z_one, z_two)]
        done, n_all = exchange(crops, (mask_one, mask_two),
                                (in_row, w_a_gate, w_a, w_b_gate, w_b, w_gate, w_out, ln_out_scale[None, :]),
                                col_count, nx, cores)
        outs = finish(crops[1], done, n_all, cores, in_row, w_gate, w_out)
        return tuple(jnp.transpose(o, (0, 2, 1)) for o in outs)

    return jax.shard_map(
        device_fn,
        mesh=mesh,
        in_specs=(pair_spec, pair_spec, mask_spec, mask_spec) + (replicated,) * 8,
        out_specs=(pair_spec, pair_spec),
        check_vma=False,
    )
```

```python
import functools
import jax
import jax.numpy as jnp
from jax import lax
from jax.experimental import pallas as pl
from jax.experimental.pallas import tpu as pltpu
from jax.sharding import PartitionSpec as P

MESH = pl.DeviceIdType.MESH
F32 = jnp.float32
BF16 = jnp.bfloat16
EPS = 1e-5
STEPS = 2
ROWS = 16
VMEM_LIMIT = 60 * 1024 * 1024
ORDER = (
    'proj', 'proj', 'bx', 'b_start', 'proj', 'proj', 'xfwd', 'proj', 'b_fwd', 'a_relay', 'a_dir', 'bx', 'bx', 'bx', 'b_start',
    'a_fwd', 'xfwd', 'xfwd', 'b_fwd', 'xfar', 'proj', 'proj', 'a_dir', 'xfwd', 'xfar', 'b_start', 'bx', 'bx', 'bx', 'bx',
    'load_a', 'proj', 'b_fwd', 'a_relay', 'a_dir', 'xfwd', 'xfwd', 'bx', 'xfar', 'xfar', 'xfwd', 'load', 'xfar', 'xfwd', 'a_dir',
    'b_start', 'xfwd', 'load2', 'bx', 'bx', 'bx', 'xfar', 'bx', 'con', 'con2', 'xfar', 'load', 'xfar', 'con2', 'load2', 'b_fwd',
    'con', 'con2', 'rs2', 'rs2', 'a_fwd', 'con2', 'xfar', 'red', 'red', 'xfwd', 'load_a', 'xfwd', 'xfwd', 'ag2', 'rs2', 'rs2',
    'red', 'norm', 'ag2', 'ag2', 'bx', 'red', 'nfwd', 'bx', 'xfar', 'xfar', 'xfar', 'load', 'load2', 'ag2', 'norm', 'norm',
    'con', 'nfwd', 'con2', 'nwait', 'xfwd', 'xfwd', 'norm', 'con2', 'rs2', 'rs2', 'nfwd', 'red', 'xfar', 'xfwd', 'red', 'nfwd',
    'nwait', 'nwait', 'bx', 'xfar', 'ag2', 'ag2', 'fin', 'xfar', 'fin', 'nwait', 'load', 'norm', 'norm', 'fin', 'xfwd', 'con',
    'nfwd', 'nfwd', 'xfar', 'load2', 'con2', 'rs2', 'con2', 'nwait', 'red', 'rs2', 'ag2', 'norm', 'fin', 'red', 'nfwd', 'ag2',
    'nwait', 'nwait', 'fin', 'norm', 'fin', 'nfwd', 'nwait',
)


def normalise_row(row, scale):
    values = row.astype(F32)
    count = values.shape[0]
    mean = jnp.sum(values, axis=0, keepdims=True) / count
    centered = values - mean
    variance = jnp.sum(centered * centered, axis=0, keepdims=True) / count
    return (centered * lax.rsqrt(variance + EPS) * scale).astype(BF16)


def transposed(ref):
    return jnp.transpose(ref[...].astype(F32), (1, 0)).astype(BF16)


def store_weights(in_ref, w_refs, in_col, w_in):
    ch, cols = in_col.shape
    in_col[...] = jnp.transpose(jnp.broadcast_to(in_ref[...].astype(F32), (cols, ch)), (1, 0))
    for k, ref in enumerate(w_refs):
        w_in[k * ref.shape[1]:(k + 1) * ref.shape[1], :] = transposed(ref)


def merge_lanes(dst, at, blocks, cores):
    pieces = [jnp.transpose(b.astype(F32), (1, 0, 2)) for b in blocks]
    part = pieces[0].shape[2] // cores
    order = [p[:, :, r * part:(r + 1) * part] for r in range(cores) for p in pieces]
    dst[:, at:at + 8, :] = jnp.concatenate(order, axis=2)


def finish_row(row, summed, scale, w_gate, w_out):
    normed = normalise_row(row, scale)
    gate = jax.nn.sigmoid(jnp.dot(w_gate, normed, preferred_element_type=F32))
    update = jnp.dot(w_out, summed.astype(BF16), preferred_element_type=F32)
    return (row.astype(F32) + gate * update).astype(BF16)


def finish_kernel(cores, done_one, done_two, z_ref, n_ref, in_ref, w_gate_ref, w_out_ref, one_ref, two_ref, sn, w_fin, in_col):
    rows, ch, cols = z_ref.shape
    steps, hid, _, lanes = n_ref.shape

    @pl.when(pl.program_id(0) == 0)
    def _():
        store_weights(in_ref, (w_gate_ref, w_out_ref), in_col, w_fin)

    one_ref[...] = done_one[...]
    two_ref[0] = done_two[...]
    for e in range(0, hid, 8):
        merge_lanes(sn, e, [n_ref[s, e:e + 8] for s in range(steps)], cores)

    def one_row(i, carry):
        two_ref[1, i] = finish_row(z_ref[i], sn[i], in_col[...], w_fin[:ch], w_fin[ch:])
        return carry

    lax.fori_loop(0, rows, one_row, 0, unroll=min(4, rows))


def finish(z_t, done, n_all, cores, in_row, w_gate, w_out):
    rows, ch, cols = z_t.shape
    hid, lanes = n_all.shape[1], n_all.shape[3]
    hp = rows // 2
    chunk = min(ROWS // 2, hp)
    steps = hp // chunk
    one, two = pl.pallas_call(
        functools.partial(finish_kernel, cores),
        grid=(steps,),
        in_specs=[
            pl.BlockSpec((2 * chunk, ch, cols), lambda i: (i, 0, 0)),
            pl.BlockSpec((chunk, ch, cols), lambda i: (2 * steps + i, 0, 0)),
            pl.BlockSpec((chunk, ch, cols), lambda i: (steps + i, 0, 0)),
            pl.BlockSpec((STEPS, hid, chunk, lanes), lambda i: (1, 0, steps + i, 0)),
            pl.BlockSpec((1, ch), lambda i: (0, 0)),
            pl.BlockSpec((ch, ch), lambda i: (0, 0)),
            pl.BlockSpec((hid, ch), lambda i: (0, 0)),
        ],
        out_specs=[
            pl.BlockSpec((2 * chunk, ch, cols), lambda i: (i, 0, 0)),
            pl.BlockSpec((2, chunk, ch, cols), lambda i: (0, i, 0, 0)),
        ],
        out_shape=[jax.ShapeDtypeStruct((rows, ch, cols), BF16), jax.ShapeDtypeStruct((2, hp, ch, cols), BF16)],
        scratch_shapes=[pltpu.VMEM((chunk, hid, cols), F32), pltpu.VMEM((2 * ch, ch), BF16), pltpu.VMEM((ch, cols), F32)],
        name="finish",
    )(done, done, z_t, n_all, in_row, w_gate, w_out)
    return one, two.reshape(rows, ch, cols)


def exchange_kernel(ny, nx, cores, z0, z1, mask0, mask1, in_ref, wag_ref, wa_ref, wbg_ref, wb_ref, wg_ref, wo_ref, out_ref,
                    done, n_out, a_all, a_relay, by, b_relay, bx, bo, n_relay, a_in, b_in,
                    a_v, b_v, o_v, ssum, st, st_rx, st_in, mr, mr_in, nv, zbuf, sa, sb, obuf, nbuf, fbuf, w_in, w_fin, in_col, out_col,
                    send_sems, recv_sems, loc_sems):
    crops = 2
    z_in, mask_in = (z0, z1), (mask0, mask1)
    cb, rows, lanes = o_v.shape[2:]
    cols = a_v.shape[3]
    sub = lanes // cores
    hid = cb * ny
    half = cb // 2
    hp = rows // 2
    hr = hp // 2
    group = zbuf.shape[1]
    groups = rows // group
    per_step = groups // STEPS
    chunk = sa.shape[0]
    y = lax.axis_index("col")
    row_id = lax.axis_index("row")
    x, r = row_id // cores, row_id % cores
    yy = [lax.rem(y + d, ny) for d in range(ny)]
    to_y = [{"col": yy[d]} for d in range(ny)]
    both_y = ((0, to_y[1]), (1, to_y[3]))
    to_x = [{"row": lax.rem(x + e, nx) * cores + r} for e in range(nx)]
    to_p = {"row": x * cores + (cores - 1 - r)}
    e_of = [lax.rem(y + d + nx - x, nx) for d in range(ny)]

    slots = {}

    def slot_of(*key):
        return slots.setdefault(key, len(slots))

    def local(src, dst, *key):
        copy = pltpu.make_async_copy(src, dst, loc_sems.at[slot_of(*key)])
        copy.start()
        return copy

    def load_z(g):
        t, h = divmod(g, groups)
        return local(z_in[t].at[pl.ds(h * group, group)], zbuf.at[g % 2], "z", g % 2)

    barrier = pltpu.get_barrier_semaphore()
    peers = [to_y[1], to_y[3], to_x[1], to_x[3], to_p]
    for dev in peers:
        pl.semaphore_signal(barrier, inc=1, device_id=dev, device_id_type=MESH)
    started = []

    def send(src, dst, dev, out, into):
        if not started:
            pl.semaphore_wait(barrier, len(peers))
        started.append(out)
        pltpu.make_async_remote_copy(
            src_ref=src, dst_ref=dst, send_sem=send_sems.at[out_of(*out)], recv_sem=recv_sems.at[into_of(*into)],
            device_id=dev, device_id_type=MESH).start()

    def out_of(*key):
        return outs_used.setdefault(key, len(outs_used))

    def into_of(*key):
        return into_used.setdefault(key, len(into_used))

    outs_used, into_used = {}, {}

    def arrived(ref, *key):
        pltpu.make_async_remote_copy(
            src_ref=ref, dst_ref=ref, send_sem=send_sems.at[0], recv_sem=recv_sems.at[into_of(*key)],
            device_id=to_p, device_id_type=MESH).wait_recv()

    def departed(ref, *key):
        pltpu.make_async_remote_copy(
            src_ref=ref, dst_ref=ref, send_sem=send_sems.at[out_of(*key)], recv_sem=recv_sems.at[0],
            device_id=to_p, device_id_type=MESH).wait_send()

    z_copy = {0: load_z(0)}
    early = (0, 1, 3)
    turns = {}

    def turn(*key):
        turns[key] = turns.get(key, -1) + 1
        return turns[key]

    def x_turn(name):
        q, k = divmod(turn(name), ny)
        return q, (*early, 2)[k]

    stored = {}
    store_weights(in_ref, (wag_ref, wa_ref, wbg_ref, wb_ref), in_col, w_in)
    for k, ref in enumerate((wg_ref, wo_ref)):
        w_fin[k] = transposed(ref)
    out_col[...] = jnp.transpose(jnp.broadcast_to(out_ref[...].astype(F32), (lanes, hid)), (1, 0))

    def wait_stored(g):
        for copy in stored.pop(g, ()):
            copy.wait()

    def op_proj():
        g = turn("proj")
        t, h = divmod(g, groups)
        z_copy[g].wait()
        if g + 1 < crops * groups:
            z_copy[g + 1] = load_z(g + 1)
        wait_stored(g - 2)
        slot = g % 2

        def one_chunk(k, carry):
            def one_row(i, inner):
                row = k * chunk + i
                normed = normalise_row(zbuf[slot, row], in_col[...])
                prod = jnp.dot(w_in[...], normed, preferred_element_type=F32)
                mask = mask_in[t][pl.ds(h * group + row, 1), :].astype(F32)
                sa[i] = mask * jax.nn.sigmoid(prod[:hid]) * prod[hid:2 * hid]
                sb[i] = mask * jax.nn.sigmoid(prod[2 * hid:3 * hid]) * prod[3 * hid:]
                return inner

            lax.fori_loop(0, chunk, one_row, 0, unroll=min(4, chunk))
            place = pl.ds(pl.multiple_of(k * chunk, chunk), chunk)
            for e in range(0, hid, 8):
                obuf[slot, 0, e:e + 8, place, :] = jnp.transpose(sa[:, e:e + 8, :], (1, 0, 2)).astype(BF16)
                obuf[slot, 1, e:e + 8, place, :] = jnp.transpose(sb[:, e:e + 8, :], (1, 0, 2)).astype(BF16)
            return carry

        lax.fori_loop(0, group // chunk, one_chunk, 0)
        s, part = divmod(h, per_step)
        stored[g] = (
            local(obuf.at[slot, 0], a_in.at[t, :, pl.ds(h * group, group), :], "a", slot),
            local(obuf.at[slot, 1], b_in.at[t, s, :, pl.ds(part * group, group), :], "b", slot),
        )

    def a_piece(t, d):
        return a_in.at[t, pl.ds(yy[d] * cb, cb)]

    def b_piece(q, d):
        t, s = divmod(q, STEPS)
        return b_in.at[t, s, pl.ds(yy[d] * cb, cb)]

    def own_piece(q, e, d):
        if e == 0:
            return b_piece(q, 0) if d == 0 else by.at[q, d - 1]
        return bx.at[q, e - 1, d]

    def ready_rows(t, first, last):
        for h in range(first, last):
            wait_stored(t * groups + h)

    def op_a_relay():
        t = turn("a_relay")
        ready_rows(t, 0, groups)
        far = a_piece(t, 2)
        for k, dev in both_y:
            send(far.at[pl.ds(k * half, half)], a_relay.at[t, k], dev, ("ar", t), ("ar", t))

    def op_a_dir():
        t, k = divmod(turn("a_dir"), 2)
        part = pl.ds(k * half, half)
        send(a_piece(t, 1).at[part], a_all.at[t, 2, part], to_y[1], ("a", t), ("a", t))
        send(a_piece(t, 3).at[part], a_all.at[t, 0, part], to_y[3], ("a", t), ("a", t))

    def op_a_fwd():
        t = turn("a_fwd")
        arrived(a_relay.at[t], "ar", t)
        for k, dev in both_y:
            send(a_relay.at[t, k], a_all.at[t, 1, pl.ds(k * half, half)], dev, ("a", t), ("a", t))

    def op_b_start():
        q = turn("b_start")
        t, s = divmod(q, STEPS)
        ready_rows(t, s * per_step, (s + 1) * per_step)
        far = b_piece(q, 2)
        for k, dev in both_y:
            send(far.at[pl.ds(k * half, half)], b_relay.at[q, k], dev, ("br", q), ("br", q))
        send(b_piece(q, 1), by.at[q, 2], to_y[1], ("b", q), ("b", q, 3))
        send(b_piece(q, 3), by.at[q, 0], to_y[3], ("b", q), ("b", q, 1))

    def op_b_fwd():
        q = turn("b_fwd")
        arrived(b_relay.at[q], "br", q)
        for k, dev in both_y:
            send(b_relay.at[q, k], by.at[q, 1, pl.ds(k * half, half)], dev, ("b", q), ("b", q, 2))

    def cross(q, e, d):
        send(own_piece(q, e, d), bo.at[q, e, d], to_p, ("c", q), ("c", q, d))

    def op_bx():
        q, d = x_turn("bx")
        t, s = divmod(q, STEPS)
        if d == 0:
            ready_rows(t, s * per_step, (s + 1) * per_step)
        else:
            arrived(by.at[q, d - 1], "b", q, d)
        send(own_piece(q, 0, d), bx.at[q, 2, d], to_x[1], ("x", q), ("x", q, d))
        send(own_piece(q, 0, d), bx.at[q, 0, d], to_x[3], ("x", q), ("x", q, d))
        cross(q, 0, d)

    def op_xfwd():
        q, d = x_turn("xfwd")
        arrived(bx.at[q, pl.ds(0, 2), d], "x", q, d)
        for k, e in enumerate((3, 1)):
            part = pl.ds(k * half, half)
            send(bx.at[q, e - 1, d, part], bx.at[q, 1, d, part], to_x[4 - e], ("x", q), ("xf", q, d))
        for e in (3, 1):
            cross(q, e, d)

    def op_xfar():
        q, d = x_turn("xfar")
        arrived(bx.at[q, 1, d], "xf", q, d)
        cross(q, 2, d)

    loads = {}

    def load_b(q, ks):
        copies = []
        for d in ks:
            for e in range(nx):
                dst = pl.ds(pl.multiple_of(e * lanes + r * sub, sub), sub)
                copies.append(local(own_piece(q, e, d), b_v.at[d, :, dst, :], "own", e, d))
        for d in ks:
            arrived(bo.at[q, :, d], "c", q, d)
            for e in range(nx):
                dst = pl.ds(pl.multiple_of(e * lanes + (cores - 1 - r) * sub, sub), sub)
                copies.append(local(bo.at[q, e, d], b_v.at[d, :, dst, :], "other", e, d))
        return copies

    def op_load():
        q = turn("load")
        loads["b", q] = load_b(q, early)

    def op_load2():
        q = turn("load2")
        loads["b2", q] = load_b(q, (2,))

    def op_load_a():
        t = turn("load_a")
        copies = [local(a_piece(t, 0), a_v.at[0], "av", 0)]
        arrived(a_all.at[t], "a", t)
        for d in (1, 3, 2):
            copies.append(local(a_all.at[t, d - 1], a_v.at[d], "av", d))
        loads["a", t] = copies

    def product(c, ks, rs):
        acc = None
        for d in ks:
            term = lax.dot_general(a_v[d, c, rs, :], b_v[d, c], (((1,), (1,)), ((), ())), preferred_element_type=F32)
            acc = term if acc is None else acc + term
        return acc

    def op_con():
        q = turn("con")
        if q % STEPS == 0:
            for copy in loads["a", q // STEPS]:
                copy.wait()
        for copy in loads["b", q]:
            copy.wait()
        slot = q % 2

        def channel(c, carry):
            acc = product(c, early, pl.ds(0, rows))
            for e in range(nx):
                o_v[slot, e, c] = acc[:, e * lanes:(e + 1) * lanes]
            return carry

        lax.fori_loop(0, cb, channel, 0)

    def op_con2():
        u = turn("con2")
        q, p = divmod(u, 2)
        if p == 0:
            for copy in loads["b2", q]:
                copy.wait()
        slot = q % 2
        rp = pl.ds(p * hp, hp)
        ssum[...] = jnp.zeros_like(ssum)

        def channel(c, carry):
            acc = product(c, (2,), rp)
            for e in range(nx):
                part = o_v[slot, e, c, rp, :] + acc[:, e * lanes:(e + 1) * lanes]
                o_v[slot, e, c, rp, :] = part
                ssum[e] += part
            return carry

        lax.fori_loop(0, cb, channel, 0)
        block = min(16, hr)

        def squares(k, carry, h):
            rs = pl.ds(pl.multiple_of(h * hr + k * block, block), block)
            ro = pl.ds(pl.multiple_of(p * hp + h * hr + k * block, block), block)
            rh = pl.ds(pl.multiple_of(k * block, block), block)
            for e in range(nx):
                total = ssum[e, rs, :]
                mean = total * (1.0 / cb)
                acc = jnp.zeros_like(mean)
                for c in range(cb):
                    diff = o_v[slot, e, c, ro, :] - mean
                    acc = acc + diff * diff
                st[u, e, h, 0, rh, :] = total
                st[u, e, h, 1, rh, :] = acc
            return carry

        for h in range(2):
            lax.fori_loop(0, hr // block, functools.partial(squares, h=h), 0)
        for k, dev in both_y:
            send(st.at[u, e_of[2], k], st_rx.at[u, k], dev, ("s", u), ("s", u))

    def op_rs2():
        u = turn("rs2")
        arrived(st_rx.at[u], "s", u)
        for k, d in ((0, 1), (1, 3)):
            e = e_of[d]
            got_sum, got_sq = st_rx[u, k, 0], st_rx[u, k, 1]
            my_sum, my_sq = st[u, e, k, 0], st[u, e, k, 1]
            diff = (my_sum - got_sum) * (1.0 / cb)
            st[u, e, k, 0] = my_sum + got_sum
            st[u, e, k, 1] = my_sq + got_sq + (0.5 * cb) * (diff * diff)
            send(st.at[u, e], st_in.at[u, k], to_y[d], ("s", u), ("t", u))

    def op_red():
        u = turn("red")
        arrived(st_in.at[u], "t", u)
        for h in range(2):
            parts = [(st[u, e_of[0], h, 0], st[u, e_of[0], h, 1], cb)]
            for k in range(2):
                parts.append((st_in[u, k, h, 0], st_in[u, k, h, 1], 2 * cb if k == h else cb))
            mean = (parts[0][0] + parts[1][0] + parts[2][0]) * (1.0 / hid)
            m2 = jnp.zeros_like(mean)
            for total, sq, n in parts:
                diff = total * (1.0 / n) - mean
                m2 = m2 + sq + n * (diff * diff)
            mr[u, h, 0] = mean
            mr[u, h, 1] = lax.rsqrt(m2 * (1.0 / hid) + EPS)
        send(mr.at[u], mr_in.at[u, 2], to_y[1], ("m", u), ("m", u))
        send(mr.at[u], mr_in.at[u, 0], to_y[3], ("m", u), ("m", u))

    def apply_norm(u, d):
        q, p = divmod(u, 2)
        e = e_of[d]
        for h in range(2):
            src = mr.at[u, h] if d == 0 else mr_in.at[u, d - 1, h]
            mean, rstd = src[0], src[1]

            def channel(c, carry, mean=mean, rstd=rstd, h=h):
                scale = out_col[pl.ds(y * cb + c, 1), :]
                value = (o_v[q % 2, e, c, pl.ds(p * hp + h * hr, hr), :] - mean) * rstd * scale
                nv[u, d, c, pl.ds(h * hr, hr), :] = value.astype(BF16)
                return carry

            lax.fori_loop(0, cb, channel, 0)

    def n_place(u, owner, *part):
        q, p = divmod(u, 2)
        return n_out.at[q, owner, *(part or (slice(None),)), pl.ds(p * hp, hp), :]

    keep = {}

    def op_ag2():
        u = turn("ag2")
        arrived(mr_in.at[u, pl.ds(0, 2)], "m", u)
        send(mr_in.at[u, 2, 0], mr_in.at[u, 1, 0], to_y[1], ("m", u), ("mf", u))
        send(mr_in.at[u, 0, 1], mr_in.at[u, 1, 1], to_y[3], ("m", u), ("mf", u))
        for d in (1, 3, 0):
            apply_norm(u, d)
        send(nv.at[u, 1], n_place(u, y), to_y[1], ("n", u), ("n", u))
        send(nv.at[u, 3], n_place(u, y), to_y[3], ("n", u), ("n", u))
        keep[u] = local(nv.at[u, 0], n_place(u, y), "keep", u)

    def op_norm():
        u = turn("norm")
        arrived(mr_in.at[u, 1], "mf", u)
        apply_norm(u, 2)
        for k, dev in both_y:
            send(nv.at[u, 2, pl.ds(k * half, half)], n_relay.at[u, k], dev, ("nr", u), ("nr", u))

    def op_nfwd():
        u = turn("nfwd")
        arrived(n_relay.at[u], "nr", u)
        for k, dev in both_y:
            owner = yy[3] if k == 0 else yy[1]
            send(n_relay.at[u, k], n_place(u, owner, pl.ds(k * half, half)), dev, ("n", u), ("n", u))

    def op_nwait():
        u = turn("nwait")
        arrived(nv.at[u, pl.ds(0, 3)], "n", u)
        keep[u].wait()

    def op_fin():
        f = turn("fin")
        t, h = divmod(f, groups)
        place = pl.ds(h * group, group)
        wait_stored(crops * groups - 2)
        wait_stored(crops * groups - 1)
        copies = [local(z_in[t].at[place], zbuf.at[0], "z", 0)]
        for s in range(STEPS):
            copies.append(local(n_out.at[t * STEPS + s, :, :, place, :], nbuf.at[s], "n", s))
        for copy in copies:
            copy.wait()
        if f:
            keep["f"].wait()

        def one_chunk(k, carry):
            at = pl.ds(pl.multiple_of(k * chunk, chunk), chunk)
            for blk in range(ny):
                for e in range(0, cb, 8):
                    merge_lanes(sa, blk * cb + e, [nbuf[s, blk, e:e + 8, at, :] for s in range(STEPS)], cores)

            def one_row(i, inner):
                row = k * chunk + i
                fbuf[row] = finish_row(zbuf[0, row], sa[i], in_col[...], w_fin[0], w_fin[1])
                return inner

            lax.fori_loop(0, chunk, one_row, 0, unroll=min(4, chunk))
            return carry

        lax.fori_loop(0, group // chunk, one_chunk, 0)
        keep["f"] = local(fbuf, done.at[pl.ds(f * group, group)], "f")

    table = dict(proj=op_proj, a_relay=op_a_relay, a_dir=op_a_dir, a_fwd=op_a_fwd, b_start=op_b_start, b_fwd=op_b_fwd,
                 bx=op_bx, xfwd=op_xfwd, xfar=op_xfar, load=op_load, load_a=op_load_a, load2=op_load2, con=op_con, con2=op_con2, rs2=op_rs2,
                 red=op_red, ag2=op_ag2, norm=op_norm, nfwd=op_nfwd, nwait=op_nwait, fin=op_fin)
    for name in ORDER:
        with jax.named_scope(name):
            table[name]()
    keep["f"].wait()
    for t in range(crops):
        departed(a_relay.at[t], "ar", t)
        departed(a_all.at[t], "a", t)
    for q in range(crops * STEPS):
        departed(b_relay.at[q], "br", q)
        departed(by.at[q], "b", q)
        departed(bx.at[q], "x", q)
        departed(bo.at[q], "c", q)
    for u in range(2 * crops * STEPS):
        departed(mr_in.at[u], "s", u)
        departed(mr_in.at[u], "m", u)
        departed(n_relay.at[u], "nr", u)
        departed(nv.at[u, pl.ds(0, 3)], "n", u)


def exchange(crops, masks, rows_in, ny, nx, cores):
    rows, ch, cols = crops[0].shape
    hid = rows_in[-1].shape[1]
    cb = hid // ny
    sub = rows // STEPS
    lanes = cores * sub
    hp = rows // 2
    hr = hp // 2
    q = 2 * STEPS
    u = 2 * q
    group = rows // 4
    chunk = min(ROWS, group)
    any_spec = pl.BlockSpec(memory_space=pl.ANY)
    vmem = pl.BlockSpec(memory_space=pltpu.VMEM)

    def hbm(*shape):
        return jax.ShapeDtypeStruct(shape, BF16)

    sends = 2 * 2 + q * 4 + u * 4
    arrivals = 2 * 2 + q * (4 + 3 * ny) + u * 6
    locals_ = 6 + 2 * nx * ny + ny + u + STEPS + 1
    outs = pl.pallas_call(
        functools.partial(exchange_kernel, ny, nx, cores),
        in_specs=[any_spec] * 2 + [vmem] * (2 + len(rows_in)),
        out_specs=[any_spec] * 11,
        out_shape=[
            hbm(rows + hp, ch, cols),
            hbm(q, ny, cb, rows, lanes),
            hbm(2, ny - 1, cb, rows, cols),
            hbm(2, 2, cb // 2, rows, cols),
            hbm(q, ny - 1, cb, sub, cols),
            hbm(q, 2, cb // 2, sub, cols),
            hbm(q, nx - 1, ny, cb, sub, cols),
            hbm(q, nx, ny, cb, sub, cols),
            hbm(u, 2, cb // 2, hp, lanes),
            hbm(2, hid, rows, cols),
            hbm(2, STEPS, hid, sub, cols),
        ],
        scratch_shapes=[
            pltpu.VMEM((ny, cb, rows, cols), BF16),
            pltpu.VMEM((ny, cb, nx * lanes, cols), BF16),
            pltpu.VMEM((2, nx, cb, rows, lanes), F32),
            pltpu.VMEM((nx, hp, lanes), F32),
            pltpu.VMEM((u, nx, 2, 2, hr, lanes), F32),
            pltpu.VMEM((u, 2, 2, hr, lanes), F32),
            pltpu.VMEM((u, 2, 2, 2, hr, lanes), F32),
            pltpu.VMEM((u, 2, 2, hr, lanes), F32),
            pltpu.VMEM((u, ny - 1, 2, 2, hr, lanes), F32),
            pltpu.VMEM((u, ny, cb, hp, lanes), BF16),
            pltpu.VMEM((2, group, ch, cols), BF16),
            pltpu.VMEM((chunk, hid, cols), F32),
            pltpu.VMEM((chunk, hid, cols), F32),
            pltpu.VMEM((2, 2, hid, group, cols), BF16),
            pltpu.VMEM((STEPS, ny, cb, group, lanes), BF16),
            pltpu.VMEM((group, ch, cols), BF16),
            pltpu.VMEM((4 * hid, ch), BF16),
            pltpu.VMEM((2, ch, hid), BF16),
            pltpu.VMEM((ch, cols), F32),
            pltpu.VMEM((hid, lanes), F32),
            pltpu.SemaphoreType.DMA((sends,)),
            pltpu.SemaphoreType.DMA((arrivals,)),
            pltpu.SemaphoreType.DMA((locals_,)),
        ],
        compiler_params=pltpu.CompilerParams(collective_id=0, has_side_effects=True, vmem_limit_bytes=VMEM_LIMIT),
        cost_estimate=pl.CostEstimate(flops=4 * rows * cols * hid * nx * cols, bytes_accessed=200000000, transcendentals=0),
        name="exchange",
    )(*crops, *masks, *rows_in)
    return outs[0], outs[1].reshape(q, hid, rows, lanes)


def solution(mesh):
    row_count = mesh.shape['row']
    col_count = mesh.shape['col']
    cores = row_count // col_count
    nx = row_count // cores
    pair_spec = P(('batch', 'row'), 'col', None)
    mask_spec = P(('batch', 'row'), 'col')
    replicated = P()

    def device_fn(z_one, z_two, mask_one, mask_two, ln_in_scale, w_a, w_a_gate, w_b, w_b_gate, w_gate, w_out, ln_out_scale):
        in_row = ln_in_scale[None, :]
        crops = [jnp.transpose(z, (0, 2, 1)) for z in (z_one, z_two)]
        done, n_all = exchange(crops, (mask_one, mask_two),
                                (in_row, w_a_gate, w_a, w_b_gate, w_b, w_gate, w_out, ln_out_scale[None, :]),
                                col_count, nx, cores)
        outs = finish(crops[1], done, n_all, cores, in_row, w_gate, w_out)
        return tuple(jnp.transpose(o, (0, 2, 1)) for o in outs)

    return jax.shard_map(
        device_fn,
        mesh=mesh,
        in_specs=(pair_spec, pair_spec, mask_spec, mask_spec) + (replicated,) * 8,
        out_specs=(pair_spec, pair_spec),
        check_vma=False,
    )
```

```python
import functools
import jax
import jax.numpy as jnp
from jax import lax
from jax.experimental import pallas as pl
from jax.experimental.pallas import tpu as pltpu
from jax.sharding import PartitionSpec as P

MESH = pl.DeviceIdType.MESH
F32 = jnp.float32
BF16 = jnp.bfloat16
EPS = 1e-5
STEPS = 2
ROWS = 16
VMEM_LIMIT = 60 * 1024 * 1024
ORDER = (
    'proj', 'proj', 'bx', 'b_start', 'xfwd', 'b_fwd', 'proj', 'bx', 'bx', 'proj', 'b_start', 'a_relay', 'proj', 'proj', 'bx',
    'bx', 'proj', 'xfar', 'b_fwd', 'a_fwd', 'proj', 'a_relay', 'xfwd', 'xfwd', 'bx', 'a_dir', 'bx', 'b_start', 'xfar', 'xfar',
    'load', 'a_dir', 'bx', 'xfwd', 'xfwd', 'xfar', 'a_fwd', 'a_dir', 'xfwd', 'xfwd', 'xfwd', 'xfar', 'xfar', 'load2', 'bx',
    'b_fwd', 'bx', 'xfar', 'load3', 'bx', 'b_start', 'load_a', 'con', 'con2', 'load', 'xfar', 'con', 'con3', 'con3', 'a_dir',
    'rs2', 'b_fwd', 'xfwd', 'bx', 'load2', 'con2', 'xfwd', 'xfwd', 'red', 'load3', 'con3', 'rs2', 'red', 'rs2', 'xfar', 'ag2',
    'ag2', 'xfwd', 'xfar', 'con3', 'load_a', 'red', 'bx', 'xfar', 'xfar', 'load3', 'bx', 'bx', 'load2', 'norm', 'load', 'nfwd',
    'rs2', 'norm', 'con', 'nwait', 'red', 'ag2', 'con2', 'con3', 'con3', 'rs2', 'rs2', 'xfwd', 'norm', 'red', 'xfwd', 'red',
    'ag2', 'ag2', 'ag2', 'norm', 'xfwd', 'nfwd', 'nfwd', 'norm', 'bx', 'xfar', 'xfar', 'xfar', 'load', 'norm', 'xfwd', 'con',
    'load2', 'nfwd', 'xfar', 'load3', 'nfwd', 'nfwd', 'con2', 'con3', 'nwait', 'con3', 'nwait', 'rs2', 'rs2', 'nwait', 'nwait',
    'red', 'red', 'ag2', 'fin', 'norm', 'nwait', 'ag2', 'fin', 'fin', 'nfwd', 'fin', 'norm', 'nwait', 'fin', 'nfwd', 'fin',
    'nwait',
)


def normalise_row(row, scale):
    values = row.astype(F32)
    count = values.shape[0]
    mean = jnp.sum(values, axis=0, keepdims=True) / count
    centered = values - mean
    variance = jnp.sum(centered * centered, axis=0, keepdims=True) / count
    return (centered * lax.rsqrt(variance + EPS) * scale).astype(BF16)


def transposed(ref):
    return jnp.transpose(ref[...].astype(F32), (1, 0)).astype(BF16)


def store_weights(in_ref, w_refs, in_col, w_in):
    ch, cols = in_col.shape
    in_col[...] = jnp.transpose(jnp.broadcast_to(in_ref[...].astype(F32), (cols, ch)), (1, 0))
    for k, ref in enumerate(w_refs):
        w_in[k * ref.shape[1]:(k + 1) * ref.shape[1], :] = transposed(ref)


def merge_lanes(dst, at, blocks, cores):
    pieces = [jnp.transpose(b.astype(F32), (1, 0, 2)) for b in blocks]
    part = pieces[0].shape[2] // cores
    order = [p[:, :, r * part:(r + 1) * part] for r in range(cores) for p in pieces]
    dst[:, at:at + 8, :] = jnp.concatenate(order, axis=2)


def finish_row(row, summed, scale, w_gate, w_out):
    normed = normalise_row(row, scale)
    gate = jax.nn.sigmoid(jnp.dot(w_gate, normed, preferred_element_type=F32))
    update = jnp.dot(w_out, summed.astype(BF16), preferred_element_type=F32)
    return (row.astype(F32) + gate * update).astype(BF16)


def finish_kernel(cores, done_one, done_two, z_ref, n_ref, in_ref, w_gate_ref, w_out_ref, one_ref, two_ref, sn, w_fin, in_col):
    rows, ch, cols = z_ref.shape
    steps, hid, _, lanes = n_ref.shape

    @pl.when(pl.program_id(0) == 0)
    def _():
        store_weights(in_ref, (w_gate_ref, w_out_ref), in_col, w_fin)

    one_ref[...] = done_one[...]
    two_ref[0] = done_two[...]
    for e in range(0, hid, 8):
        merge_lanes(sn, e, [n_ref[s, e:e + 8] for s in range(steps)], cores)

    def one_row(i, carry):
        two_ref[1, i] = finish_row(z_ref[i], sn[i], in_col[...], w_fin[:ch], w_fin[ch:])
        return carry

    lax.fori_loop(0, rows, one_row, 0, unroll=min(8, rows))


def finish(z_t, done, n_all, cores, in_row, w_gate, w_out):
    rows, ch, cols = z_t.shape
    hid, lanes = n_all.shape[1], n_all.shape[3]
    hp = rows // 2
    chunk = min(ROWS, hp)
    steps = hp // chunk
    one, two = pl.pallas_call(
        functools.partial(finish_kernel, cores),
        grid=(steps,),
        in_specs=[
            pl.BlockSpec((2 * chunk, ch, cols), lambda i: (i, 0, 0)),
            pl.BlockSpec((chunk, ch, cols), lambda i: (2 * steps + i, 0, 0)),
            pl.BlockSpec((chunk, ch, cols), lambda i: (steps + i, 0, 0)),
            pl.BlockSpec((STEPS, hid, chunk, lanes), lambda i: (1, 0, steps + i, 0)),
            pl.BlockSpec((1, ch), lambda i: (0, 0)),
            pl.BlockSpec((ch, ch), lambda i: (0, 0)),
            pl.BlockSpec((hid, ch), lambda i: (0, 0)),
        ],
        out_specs=[
            pl.BlockSpec((2 * chunk, ch, cols), lambda i: (i, 0, 0)),
            pl.BlockSpec((2, chunk, ch, cols), lambda i: (0, i, 0, 0)),
        ],
        out_shape=[jax.ShapeDtypeStruct((rows, ch, cols), BF16), jax.ShapeDtypeStruct((2, hp, ch, cols), BF16)],
        scratch_shapes=[pltpu.VMEM((chunk, hid, cols), F32), pltpu.VMEM((2 * ch, ch), BF16), pltpu.VMEM((ch, cols), F32)],
        name="finish",
    )(done, done, z_t, n_all, in_row, w_gate, w_out)
    return one, two.reshape(rows, ch, cols)


def exchange_kernel(ny, nx, cores, z0, z1, mask0, mask1, in_ref, wag_ref, wa_ref, wbg_ref, wb_ref, wg_ref, wo_ref, out_ref,
                    done, n_out, a_all, a_relay, by, b_relay, bx, bo, n_relay, a_in, b_in,
                    a_v, b_v, o_v, ssum, st, st_rx, st_in, mr, mr_in, nv, zbuf, sa, sb, obuf, nbuf, fbuf, w_in, w_fin, in_col, out_col,
                    send_sems, recv_sems, loc_sems):
    crops = 2
    z_in, mask_in = (z0, z1), (mask0, mask1)
    cb, rows, lanes = o_v.shape[2:]
    cols = a_v.shape[3]
    sub = lanes // cores
    hid = cb * ny
    half = cb // 2
    hp = rows // 2
    hr = hp // 2
    group = zbuf.shape[1]
    groups = rows // group
    per_step = groups // STEPS
    chunk = sa.shape[0]
    y = lax.axis_index("col")
    row_id = lax.axis_index("row")
    x, r = row_id // cores, row_id % cores
    yy = [lax.rem(y + d, ny) for d in range(ny)]
    to_y = [{"col": yy[d]} for d in range(ny)]
    both_y = ((0, to_y[1]), (1, to_y[3]))
    to_x = [{"row": lax.rem(x + e, nx) * cores + r} for e in range(nx)]
    to_p = {"row": x * cores + (cores - 1 - r)}
    e_of = [lax.rem(y + d + nx - x, nx) for d in range(ny)]

    slots = {}

    def slot_of(*key):
        return slots.setdefault(key, len(slots))

    def local(src, dst, *key):
        copy = pltpu.make_async_copy(src, dst, loc_sems.at[slot_of(*key)])
        copy.start()
        return copy

    def load_z(g):
        t, h = divmod(g, groups)
        return local(z_in[t].at[pl.ds(h * group, group)], zbuf.at[g % 2], "z", g % 2)

    barrier = pltpu.get_barrier_semaphore()
    peers = [to_y[1], to_y[3], to_x[1], to_x[3], to_p]
    for dev in peers:
        pl.semaphore_signal(barrier, inc=1, device_id=dev, device_id_type=MESH)
    started = []

    def send(src, dst, dev, out, into):
        if not started:
            pl.semaphore_wait(barrier, len(peers))
        started.append(out)
        pltpu.make_async_remote_copy(
            src_ref=src, dst_ref=dst, send_sem=send_sems.at[out_of(*out)], recv_sem=recv_sems.at[into_of(*into)],
            device_id=dev, device_id_type=MESH).start()

    def out_of(*key):
        return outs_used.setdefault(key, len(outs_used))

    def into_of(*key):
        return into_used.setdefault(key, len(into_used))

    outs_used, into_used = {}, {}

    def arrived(ref, *key):
        pltpu.make_async_remote_copy(
            src_ref=ref, dst_ref=ref, send_sem=send_sems.at[0], recv_sem=recv_sems.at[into_of(*key)],
            device_id=to_p, device_id_type=MESH).wait_recv()

    def departed(ref, *key):
        pltpu.make_async_remote_copy(
            src_ref=ref, dst_ref=ref, send_sem=send_sems.at[out_of(*key)], recv_sem=recv_sems.at[0],
            device_id=to_p, device_id_type=MESH).wait_send()

    z_copy = {0: load_z(0)}
    early = (0, 1, 3)
    turns = {}

    def turn(*key):
        turns[key] = turns.get(key, -1) + 1
        return turns[key]

    def x_turn(name):
        q, k = divmod(turn(name), ny)
        return q, (*early, 2)[k]

    stored = {}
    store_weights(in_ref, (wag_ref, wa_ref, wbg_ref, wb_ref), in_col, w_in)
    for k, ref in enumerate((wg_ref, wo_ref)):
        w_fin[k] = transposed(ref)
    out_col[...] = jnp.transpose(jnp.broadcast_to(out_ref[...].astype(F32), (lanes, hid)), (1, 0))

    def wait_stored(g):
        for copy in stored.pop(g, ()):
            copy.wait()

    def op_proj():
        g = turn("proj")
        t, h = divmod(g, groups)
        z_copy[g].wait()
        if g + 1 < crops * groups:
            z_copy[g + 1] = load_z(g + 1)
        wait_stored(g - 2)
        slot = g % 2

        def one_chunk(k, carry):
            def one_row(i, inner):
                row = k * chunk + i
                normed = normalise_row(zbuf[slot, row], in_col[...])
                prod = jnp.dot(w_in[...], normed, preferred_element_type=F32)
                mask = mask_in[t][pl.ds(h * group + row, 1), :].astype(F32)
                sa[i] = mask * jax.nn.sigmoid(prod[:hid]) * prod[hid:2 * hid]
                sb[i] = mask * jax.nn.sigmoid(prod[2 * hid:3 * hid]) * prod[3 * hid:]
                return inner

            lax.fori_loop(0, chunk, one_row, 0, unroll=min(8, chunk))
            place = pl.ds(pl.multiple_of(k * chunk, chunk), chunk)
            for e in range(0, hid, 8):
                obuf[slot, 0, e:e + 8, place, :] = jnp.transpose(sa[:, e:e + 8, :], (1, 0, 2)).astype(BF16)
                obuf[slot, 1, e:e + 8, place, :] = jnp.transpose(sb[:, e:e + 8, :], (1, 0, 2)).astype(BF16)
            return carry

        lax.fori_loop(0, group // chunk, one_chunk, 0)
        s, part = divmod(h, per_step)
        stored[g] = (
            local(obuf.at[slot, 0], a_in.at[t, :, pl.ds(h * group, group), :], "a", slot),
            local(obuf.at[slot, 1], b_in.at[t, s, :, pl.ds(part * group, group), :], "b", slot),
        )

    def a_piece(t, d):
        return a_in.at[t, pl.ds(yy[d] * cb, cb)]

    def b_piece(q, d):
        t, s = divmod(q, STEPS)
        return b_in.at[t, s, pl.ds(yy[d] * cb, cb)]

    def own_piece(q, e, d):
        if e == 0:
            return b_piece(q, 0) if d == 0 else by.at[q, d - 1]
        return bx.at[q, e - 1, d]

    def ready_rows(t, first, last):
        for h in range(first, last):
            wait_stored(t * groups + h)

    def op_a_relay():
        t = turn("a_relay")
        ready_rows(t, 0, groups)
        far = a_piece(t, 2)
        for k, dev in both_y:
            send(far.at[pl.ds(k * half, half)], a_relay.at[t, k], dev, ("ar", t), ("ar", t))

    def op_a_dir():
        t, k = divmod(turn("a_dir"), 2)
        part = pl.ds(k * half, half)
        send(a_piece(t, 1).at[part], a_all.at[t, 2, part], to_y[1], ("a", t), ("a", t))
        send(a_piece(t, 3).at[part], a_all.at[t, 0, part], to_y[3], ("a", t), ("a", t))

    def op_a_fwd():
        t = turn("a_fwd")
        arrived(a_relay.at[t], "ar", t)
        for k, dev in both_y:
            send(a_relay.at[t, k], a_all.at[t, 1, pl.ds(k * half, half)], dev, ("a", t), ("a", t))

    def op_b_start():
        q = turn("b_start")
        t, s = divmod(q, STEPS)
        ready_rows(t, s * per_step, (s + 1) * per_step)
        far = b_piece(q, 2)
        for k, dev in both_y:
            send(far.at[pl.ds(k * half, half)], b_relay.at[q, k], dev, ("br", q), ("br", q))
        send(b_piece(q, 1), by.at[q, 2], to_y[1], ("b", q), ("b", q, 3))
        send(b_piece(q, 3), by.at[q, 0], to_y[3], ("b", q), ("b", q, 1))

    def op_b_fwd():
        q = turn("b_fwd")
        arrived(b_relay.at[q], "br", q)
        for k, dev in both_y:
            send(b_relay.at[q, k], by.at[q, 1, pl.ds(k * half, half)], dev, ("b", q), ("b", q, 2))

    def cross(q, e, d):
        send(own_piece(q, e, d), bo.at[q, e, d], to_p, ("c", q), ("cf", q) if e == d == 2 else ("c", q, d))

    def op_bx():
        q, d = x_turn("bx")
        t, s = divmod(q, STEPS)
        if d == 0:
            ready_rows(t, s * per_step, (s + 1) * per_step)
        else:
            arrived(by.at[q, d - 1], "b", q, d)
        send(own_piece(q, 0, d), bx.at[q, 2, d], to_x[1], ("x", q), ("x", q, d))
        send(own_piece(q, 0, d), bx.at[q, 0, d], to_x[3], ("x", q), ("x", q, d))
        cross(q, 0, d)

    def op_xfwd():
        q, d = x_turn("xfwd")
        arrived(bx.at[q, pl.ds(0, 2), d], "x", q, d)
        for k, e in enumerate((3, 1)):
            part = pl.ds(k * half, half)
            send(bx.at[q, e - 1, d, part], bx.at[q, 1, d, part], to_x[4 - e], ("x", q), ("xf", q, d))
        for e in (3, 1):
            cross(q, e, d)

    def op_xfar():
        q, d = x_turn("xfar")
        arrived(bx.at[q, 1, d], "xf", q, d)
        cross(q, 2, d)

    loads = {}

    def load_b(q, ks, es):
        copies = []
        for d in ks:
            for e in es:
                dst = pl.ds(pl.multiple_of(e * lanes + r * sub, sub), sub)
                copies.append(local(own_piece(q, e, d), b_v.at[d, :, dst, :], "own", e, d))
        for d in ks:
            if len(es) == 1:
                arrived(bo.at[q, 2, d], "cf", q)
            else:
                arrived(bo.at[q, pl.ds(0, len(es)), d], "c", q, d)
            for e in es:
                dst = pl.ds(pl.multiple_of(e * lanes + (cores - 1 - r) * sub, sub), sub)
                copies.append(local(bo.at[q, e, d], b_v.at[d, :, dst, :], "other", e, d))
        return copies

    def op_load():
        q = turn("load")
        loads["b", q] = load_b(q, early, range(nx))

    def op_load2():
        q = turn("load2")
        loads["b2", q] = load_b(q, (2,), early)

    def op_load3():
        q = turn("load3")
        loads["b3", q] = load_b(q, (2,), (2,))

    def op_load_a():
        t = turn("load_a")
        copies = [local(a_piece(t, 0), a_v.at[0], "av", 0)]
        arrived(a_all.at[t], "a", t)
        for d in (1, 3, 2):
            copies.append(local(a_all.at[t, d - 1], a_v.at[d], "av", d))
        loads["a", t] = copies

    def product(c, d, rs, js):
        return lax.dot_general(a_v[d, c, rs, :], b_v[d, c, js, :], (((1,), (1,)), ((), ())), preferred_element_type=F32)

    everything = slice(None)

    def op_con():
        q = turn("con")
        if q % STEPS == 0:
            for copy in loads["a", q // STEPS]:
                copy.wait()
        for copy in loads["b", q]:
            copy.wait()
        slot = q % 2

        def channel(c, carry):
            acc = product(c, 0, everything, everything)
            for d in early[1:]:
                acc = acc + product(c, d, everything, everything)
            for e in range(nx):
                o_v[slot, e, c] = acc[:, e * lanes:(e + 1) * lanes]
            return carry

        lax.fori_loop(0, cb, channel, 0)

    def add_last(q, rs, first, count):
        slot = q % 2
        js = slice(first * lanes, (first + count) * lanes)

        def channel(c, carry):
            acc = product(c, 2, rs, js)
            for k in range(count):
                part = o_v[slot, first + k, c, rs, :] + acc[:, k * lanes:(k + 1) * lanes]
                o_v[slot, first + k, c, rs, :] = part
                ssum[first + k, rs, :] += part
            return carry

        lax.fori_loop(0, cb, channel, 0)

    def spread(u, es):
        q, p = divmod(u, 2)
        block = min(16, hr)

        def squares(k, carry, h):
            ro = pl.ds(pl.multiple_of(p * hp + h * hr + k * block, block), block)
            rh = pl.ds(pl.multiple_of(k * block, block), block)
            for e in es:
                total = ssum[e, ro, :]
                mean = total * (1.0 / cb)
                acc = jnp.zeros_like(mean)
                for c in range(cb):
                    diff = o_v[q % 2, e, c, ro, :] - mean
                    acc = acc + diff * diff
                st[u, e, h, 0, rh, :] = total
                st[u, e, h, 1, rh, :] = acc
            return carry

        for h in range(2):
            lax.fori_loop(0, hr // block, functools.partial(squares, h=h), 0)

    def op_con2():
        q = turn("con2")
        for copy in loads["b2", q]:
            copy.wait()
        ssum[...] = jnp.zeros_like(ssum)
        add_last(q, pl.ds(0, rows), 0, 2)
        add_last(q, pl.ds(0, rows), 3, 1)
        for u in (2 * q, 2 * q + 1):
            spread(u, early)

    def op_con3():
        u = turn("con3")
        q, p = divmod(u, 2)
        if p == 0:
            for copy in loads["b3", q]:
                copy.wait()
        add_last(q, pl.ds(p * hp, hp), 2, 1)
        spread(u, (2,))
        for k, dev in both_y:
            send(st.at[u, e_of[2], k], st_rx.at[u, k], dev, ("s", u), ("s", u))

    def op_rs2():
        u = turn("rs2")
        arrived(st_rx.at[u], "s", u)
        for k, d in ((0, 1), (1, 3)):
            e = e_of[d]
            got_sum, got_sq = st_rx[u, k, 0], st_rx[u, k, 1]
            my_sum, my_sq = st[u, e, k, 0], st[u, e, k, 1]
            diff = (my_sum - got_sum) * (1.0 / cb)
            st[u, e, k, 0] = my_sum + got_sum
            st[u, e, k, 1] = my_sq + got_sq + (0.5 * cb) * (diff * diff)
            send(st.at[u, e], st_in.at[u, k], to_y[d], ("s", u), ("t", u))

    def op_red():
        u = turn("red")
        arrived(st_in.at[u], "t", u)
        for h in range(2):
            parts = [(st[u, e_of[0], h, 0], st[u, e_of[0], h, 1], cb)]
            for k in range(2):
                parts.append((st_in[u, k, h, 0], st_in[u, k, h, 1], 2 * cb if k == h else cb))
            mean = (parts[0][0] + parts[1][0] + parts[2][0]) * (1.0 / hid)
            m2 = jnp.zeros_like(mean)
            for total, sq, n in parts:
                diff = total * (1.0 / n) - mean
                m2 = m2 + sq + n * (diff * diff)
            mr[u, h, 0] = mean
            mr[u, h, 1] = lax.rsqrt(m2 * (1.0 / hid) + EPS)
        send(mr.at[u], mr_in.at[u, 2], to_y[1], ("m", u), ("m", u))
        send(mr.at[u], mr_in.at[u, 0], to_y[3], ("m", u), ("m", u))

    def apply_norm(u, d):
        q, p = divmod(u, 2)
        e = e_of[d]
        for h in range(2):
            src = mr.at[u, h] if d == 0 else mr_in.at[u, d - 1, h]
            mean, rstd = src[0], src[1]

            def channel(c, carry, mean=mean, rstd=rstd, h=h):
                scale = out_col[pl.ds(y * cb + c, 1), :]
                value = (o_v[q % 2, e, c, pl.ds(p * hp + h * hr, hr), :] - mean) * rstd * scale
                nv[u, d, c, pl.ds(h * hr, hr), :] = value.astype(BF16)
                return carry

            lax.fori_loop(0, cb, channel, 0)

    def n_place(u, owner, *part):
        q, p = divmod(u, 2)
        return n_out.at[q, owner, *(part or (slice(None),)), pl.ds(p * hp, hp), :]

    keep = {}

    def op_ag2():
        u = turn("ag2")
        arrived(mr_in.at[u, pl.ds(0, 2)], "m", u)
        send(mr_in.at[u, 2, 0], mr_in.at[u, 1, 0], to_y[1], ("m", u), ("mf", u))
        send(mr_in.at[u, 0, 1], mr_in.at[u, 1, 1], to_y[3], ("m", u), ("mf", u))
        for d in (1, 3, 0):
            apply_norm(u, d)
        send(nv.at[u, 1], n_place(u, y), to_y[1], ("n", u), ("n", u))
        send(nv.at[u, 3], n_place(u, y), to_y[3], ("n", u), ("n", u))
        keep[u] = local(nv.at[u, 0], n_place(u, y), "keep", u)

    def op_norm():
        u = turn("norm")
        arrived(mr_in.at[u, 1], "mf", u)
        apply_norm(u, 2)
        for k, dev in both_y:
            send(nv.at[u, 2, pl.ds(k * half, half)], n_relay.at[u, k], dev, ("nr", u), ("nr", u))

    def op_nfwd():
        u = turn("nfwd")
        arrived(n_relay.at[u], "nr", u)
        for k, dev in both_y:
            owner = yy[3] if k == 0 else yy[1]
            send(n_relay.at[u, k], n_place(u, owner, pl.ds(k * half, half)), dev, ("n", u), ("n", u))

    def op_nwait():
        u = turn("nwait")
        arrived(nv.at[u, pl.ds(0, 3)], "n", u)
        keep[u].wait()

    def op_fin():
        f = turn("fin")
        t, h = divmod(f, groups)
        place = pl.ds(h * group, group)
        wait_stored(crops * groups - 2)
        wait_stored(crops * groups - 1)
        copies = [local(z_in[t].at[place], zbuf.at[0], "z", 0)]
        for s in range(STEPS):
            copies.append(local(n_out.at[t * STEPS + s, :, :, place, :], nbuf.at[s], "n", s))
        for copy in copies:
            copy.wait()
        if f:
            keep["f"].wait()

        def one_chunk(k, carry):
            at = pl.ds(pl.multiple_of(k * chunk, chunk), chunk)
            for blk in range(ny):
                for e in range(0, cb, 8):
                    merge_lanes(sa, blk * cb + e, [nbuf[s, blk, e:e + 8, at, :] for s in range(STEPS)], cores)

            def one_row(i, inner):
                row = k * chunk + i
                fbuf[row] = finish_row(zbuf[0, row], sa[i], in_col[...], w_fin[0], w_fin[1])
                return inner

            lax.fori_loop(0, chunk, one_row, 0, unroll=min(8, chunk))
            return carry

        lax.fori_loop(0, group // chunk, one_chunk, 0)
        keep["f"] = local(fbuf, done.at[pl.ds(f * group, group)], "f")

    table = dict(proj=op_proj, a_relay=op_a_relay, a_dir=op_a_dir, a_fwd=op_a_fwd, b_start=op_b_start, b_fwd=op_b_fwd,
                 bx=op_bx, xfwd=op_xfwd, xfar=op_xfar, load=op_load, load_a=op_load_a, load2=op_load2, load3=op_load3, con3=op_con3, con=op_con, con2=op_con2, rs2=op_rs2,
                 red=op_red, ag2=op_ag2, norm=op_norm, nfwd=op_nfwd, nwait=op_nwait, fin=op_fin)
    for name in ORDER:
        with jax.named_scope(name):
            table[name]()
    keep["f"].wait()
    for t in range(crops):
        departed(a_relay.at[t], "ar", t)
        departed(a_all.at[t], "a", t)
    for q in range(crops * STEPS):
        departed(b_relay.at[q], "br", q)
        departed(by.at[q], "b", q)
        departed(bx.at[q], "x", q)
        departed(bo.at[q], "c", q)
    for u in range(2 * crops * STEPS):
        departed(mr_in.at[u], "s", u)
        departed(mr_in.at[u], "m", u)
        departed(n_relay.at[u], "nr", u)
        departed(nv.at[u, pl.ds(0, 3)], "n", u)


def exchange(crops, masks, rows_in, ny, nx, cores):
    rows, ch, cols = crops[0].shape
    hid = rows_in[-1].shape[1]
    cb = hid // ny
    sub = rows // STEPS
    lanes = cores * sub
    hp = rows // 2
    hr = hp // 2
    q = 2 * STEPS
    u = 2 * q
    group = rows // 4
    chunk = min(ROWS, group)
    any_spec = pl.BlockSpec(memory_space=pl.ANY)
    vmem = pl.BlockSpec(memory_space=pltpu.VMEM)

    def hbm(*shape):
        return jax.ShapeDtypeStruct(shape, BF16)

    sends = 2 * 2 + q * 4 + u * 4
    arrivals = 2 * 2 + q * (5 + 3 * ny) + u * 6
    locals_ = 6 + 2 * nx * ny + ny + u + STEPS + 1
    outs = pl.pallas_call(
        functools.partial(exchange_kernel, ny, nx, cores),
        in_specs=[any_spec] * 2 + [vmem] * (2 + len(rows_in)),
        out_specs=[any_spec] * 11,
        out_shape=[
            hbm(rows + hp, ch, cols),
            hbm(q, ny, cb, rows, lanes),
            hbm(2, ny - 1, cb, rows, cols),
            hbm(2, 2, cb // 2, rows, cols),
            hbm(q, ny - 1, cb, sub, cols),
            hbm(q, 2, cb // 2, sub, cols),
            hbm(q, nx - 1, ny, cb, sub, cols),
            hbm(q, nx, ny, cb, sub, cols),
            hbm(u, 2, cb // 2, hp, lanes),
            hbm(2, hid, rows, cols),
            hbm(2, STEPS, hid, sub, cols),
        ],
        scratch_shapes=[
            pltpu.VMEM((ny, cb, rows, cols), BF16),
            pltpu.VMEM((ny, cb, nx * lanes, cols), BF16),
            pltpu.VMEM((2, nx, cb, rows, lanes), F32),
            pltpu.VMEM((nx, rows, lanes), F32),
            pltpu.VMEM((u, nx, 2, 2, hr, lanes), F32),
            pltpu.VMEM((u, 2, 2, hr, lanes), F32),
            pltpu.VMEM((u, 2, 2, 2, hr, lanes), F32),
            pltpu.VMEM((u, 2, 2, hr, lanes), F32),
            pltpu.VMEM((u, ny - 1, 2, 2, hr, lanes), F32),
            pltpu.VMEM((u, ny, cb, hp, lanes), BF16),
            pltpu.VMEM((2, group, ch, cols), BF16),
            pltpu.VMEM((chunk, hid, cols), F32),
            pltpu.VMEM((chunk, hid, cols), F32),
            pltpu.VMEM((2, 2, hid, group, cols), BF16),
            pltpu.VMEM((STEPS, ny, cb, group, lanes), BF16),
            pltpu.VMEM((group, ch, cols), BF16),
            pltpu.VMEM((4 * hid, ch), BF16),
            pltpu.VMEM((2, ch, hid), BF16),
            pltpu.VMEM((ch, cols), F32),
            pltpu.VMEM((hid, lanes), F32),
            pltpu.SemaphoreType.DMA((sends,)),
            pltpu.SemaphoreType.DMA((arrivals,)),
            pltpu.SemaphoreType.DMA((locals_,)),
        ],
        compiler_params=pltpu.CompilerParams(collective_id=0, has_side_effects=True, vmem_limit_bytes=VMEM_LIMIT),
        cost_estimate=pl.CostEstimate(flops=4 * rows * cols * hid * nx * cols, bytes_accessed=200000000, transcendentals=0),
        name="exchange",
    )(*crops, *masks, *rows_in)
    return outs[0], outs[1].reshape(q, hid, rows, lanes)


def solution(mesh):
    row_count = mesh.shape['row']
    col_count = mesh.shape['col']
    cores = row_count // col_count
    nx = row_count // cores
    pair_spec = P(('batch', 'row'), 'col', None)
    mask_spec = P(('batch', 'row'), 'col')
    replicated = P()

    def device_fn(z_one, z_two, mask_one, mask_two, ln_in_scale, w_a, w_a_gate, w_b, w_b_gate, w_gate, w_out, ln_out_scale):
        in_row = ln_in_scale[None, :]
        crops = [jnp.transpose(z, (0, 2, 1)) for z in (z_one, z_two)]
        done, n_all = exchange(crops, (mask_one, mask_two),
                                (in_row, w_a_gate, w_a, w_b_gate, w_b, w_gate, w_out, ln_out_scale[None, :]),
                                col_count, nx, cores)
        outs = finish(crops[1], done, n_all, cores, in_row, w_gate, w_out)
        return tuple(jnp.transpose(o, (0, 2, 1)) for o in outs)

    return jax.shard_map(
        device_fn,
        mesh=mesh,
        in_specs=(pair_spec, pair_spec, mask_spec, mask_spec) + (replicated,) * 8,
        out_specs=(pair_spec, pair_spec),
        check_vma=False,
    )
```

```python
import functools
import jax
import jax.numpy as jnp
from jax import lax
from jax.experimental import pallas as pl
from jax.experimental.pallas import tpu as pltpu
from jax.sharding import PartitionSpec as P

MESH = pl.DeviceIdType.MESH
F32 = jnp.float32
BF16 = jnp.bfloat16
EPS = 1e-5
STEPS = 2
ROWS = 16
VMEM_LIMIT = 60 * 1024 * 1024
ORDER = (
    'proj', 'proj', 'bx', 'b_start', 'xfwd', 'proj', 'bx', 'b_fwd', 'bx', 'proj', 'a_relay', 'a_dir', 'bx', 'xfar', 'a_dir',
    'proj', 'proj', 'b_start', 'bx', 'b_start', 'xfwd', 'xfwd', 'xfwd', 'proj', 'bx', 'b_fwd', 'xfwd', 'proj', 'xfar', 'xfar',
    'load', 'bx', 'a_fwd', 'b_start', 'load1', 'xfar', 'load2', 'xfar', 'xfwd', 'a_relay', 'a_dir', 'bx', 'load_a', 'xfwd',
    'xfar', 'con', 'b_fwd', 'b_fwd', 'bx', 'con1', 'con2', 'a_fwd', 'xfwd', 'load', 'con2', 'xfwd', 'xfar', 'bx', 'xfar', 'bx',
    'bx', 'load1', 'a_dir', 'xfar', 'con', 'con1', 'xfwd', 'xfwd', 'load2', 'rs2', 'con2', 'red', 'rs2', 'rs2', 'bx', 'xfwd',
    'ag2', 'red', 'norm', 'con2', 'bx', 'xfar', 'xfar', 'load1', 'ag2', 'rs2', 'red', 'load_a', 'red', 'norm', 'bx', 'ag2',
    'xfwd', 'load', 'ag2', 'nfwd', 'xfar', 'load2', 'con', 'con1', 'norm', 'con2', 'xfwd', 'con2', 'bx', 'rs2', 'xfwd', 'rs2',
    'nfwd', 'red', 'nwait', 'red', 'nwait', 'nfwd', 'xfar', 'norm', 'ag2', 'norm', 'xfar', 'load', 'xfwd', 'ag2', 'con', 'norm',
    'xfar', 'load1', 'xfar', 'nfwd', 'nfwd', 'load2', 'nfwd', 'con1', 'con2', 'nwait', 'con2', 'rs2', 'rs2', 'red', 'red', 'ag2',
    'ag2', 'fin', 'fin', 'norm', 'norm', 'nwait', 'fin', 'nfwd', 'nwait', 'nfwd', 'fin', 'nwait', 'nwait', 'nwait',
)


def normalise_row(row, scale):
    values = row.astype(F32)
    count = values.shape[0]
    mean = jnp.sum(values, axis=0, keepdims=True) / count
    centered = values - mean
    variance = jnp.sum(centered * centered, axis=0, keepdims=True) / count
    return (centered * lax.rsqrt(variance + EPS) * scale).astype(BF16)


def transposed(ref):
    return jnp.transpose(ref[...].astype(F32), (1, 0)).astype(BF16)


def store_weights(in_ref, w_refs, in_col, w_in):
    ch, cols = in_col.shape
    in_col[...] = jnp.transpose(jnp.broadcast_to(in_ref[...].astype(F32), (cols, ch)), (1, 0))
    for k, ref in enumerate(w_refs):
        w_in[k * ref.shape[1]:(k + 1) * ref.shape[1], :] = transposed(ref)


def merge_lanes(dst, at, blocks, cores):
    pieces = [jnp.transpose(b.astype(F32), (1, 0, 2)) for b in blocks]
    part = pieces[0].shape[2] // cores
    order = [p[:, :, r * part:(r + 1) * part] for r in range(cores) for p in pieces]
    dst[:, at:at + 8, :] = jnp.concatenate(order, axis=2)


def finish_row(row, summed, scale, w_gate, w_out):
    normed = normalise_row(row, scale)
    gate = jax.nn.sigmoid(jnp.dot(w_gate, normed, preferred_element_type=F32))
    update = jnp.dot(w_out, summed.astype(BF16), preferred_element_type=F32)
    return (row.astype(F32) + gate * update).astype(BF16)


def finish_kernel(cores, done_ref, z_ref, n_ref, in_ref, w_gate_ref, w_out_ref, one_ref, two_ref, sn, w_fin, in_col):
    rows, ch, cols = z_ref.shape
    steps, hid, _, lanes = n_ref.shape

    @pl.when(pl.program_id(0) == 0)
    def _():
        store_weights(in_ref, (w_gate_ref, w_out_ref), in_col, w_fin)

    one_ref[...] = done_ref[...]
    for e in range(0, hid, 8):
        merge_lanes(sn, e, [n_ref[s, e:e + 8] for s in range(steps)], cores)

    def one_row(i, carry):
        two_ref[i] = finish_row(z_ref[i], sn[i], in_col[...], w_fin[:ch], w_fin[ch:])
        return carry

    lax.fori_loop(0, rows, one_row, 0, unroll=min(8, rows))


def finish(z_t, done, n_all, cores, in_row, w_gate, w_out):
    rows, ch, cols = z_t.shape
    hid, lanes = n_all.shape[1], n_all.shape[3]
    chunk = min(ROWS, rows)
    block = pl.BlockSpec((chunk, ch, cols), lambda i: (i, 0, 0))
    return pl.pallas_call(
        functools.partial(finish_kernel, cores),
        grid=(rows // chunk,),
        in_specs=[
            block,
            block,
            pl.BlockSpec((STEPS, hid, chunk, lanes), lambda i: (1, 0, i, 0)),
            pl.BlockSpec((1, ch), lambda i: (0, 0)),
            pl.BlockSpec((ch, ch), lambda i: (0, 0)),
            pl.BlockSpec((hid, ch), lambda i: (0, 0)),
        ],
        out_specs=[block, block],
        out_shape=[jax.ShapeDtypeStruct((rows, ch, cols), BF16)] * 2,
        scratch_shapes=[pltpu.VMEM((chunk, hid, cols), F32), pltpu.VMEM((2 * ch, ch), BF16), pltpu.VMEM((ch, cols), F32)],
        name="finish",
    )(done, z_t, n_all, in_row, w_gate, w_out)


def exchange_kernel(ny, nx, cores, z0, z1, mask0, mask1, in_ref, wag_ref, wa_ref, wbg_ref, wb_ref, wg_ref, wo_ref, out_ref,
                    done, n_out, a_all, a_relay, by, b_relay, bx, bo, n_relay, a_in, b_in,
                    a_v, b_v, o_v, ssum, st, st_rx, st_in, mr, mr_in, nv, zbuf, sa, sb, obuf, nbuf, fbuf, w_in, w_fin, in_col, out_col,
                    send_sems, recv_sems, loc_sems):
    crops = 2
    z_in, mask_in = (z0, z1), (mask0, mask1)
    cb, rows, lanes = o_v.shape[2:]
    cols = a_v.shape[3]
    sub = lanes // cores
    hid = cb * ny
    half = cb // 2
    hp = rows // 2
    hr = hp // 2
    group = zbuf.shape[1]
    groups = rows // group
    per_step = groups // STEPS
    chunk = sa.shape[0]
    y = lax.axis_index("col")
    row_id = lax.axis_index("row")
    x, r = row_id // cores, row_id % cores
    yy = [lax.rem(y + d, ny) for d in range(ny)]
    to_y = [{"col": yy[d]} for d in range(ny)]
    both_y = ((0, to_y[1]), (1, to_y[3]))
    to_x = [{"row": lax.rem(x + e, nx) * cores + r} for e in range(nx)]
    to_p = {"row": x * cores + (cores - 1 - r)}
    e_of = [lax.rem(y + d + nx - x, nx) for d in range(ny)]

    slots = {}

    def slot_of(*key):
        return slots.setdefault(key, len(slots))

    def local(src, dst, *key):
        copy = pltpu.make_async_copy(src, dst, loc_sems.at[slot_of(*key)])
        copy.start()
        return copy

    def load_z(g):
        t, h = divmod(g, groups)
        return local(z_in[t].at[pl.ds(h * group, group)], zbuf.at[g % 2], "z", g % 2)

    barrier = pltpu.get_barrier_semaphore()
    peers = [to_y[1], to_y[3], to_x[1], to_x[3], to_p]
    for dev in peers:
        pl.semaphore_signal(barrier, inc=1, device_id=dev, device_id_type=MESH)
    started = []

    def send(src, dst, dev, out, into):
        if not started:
            pl.semaphore_wait(barrier, len(peers))
        started.append(out)
        pltpu.make_async_remote_copy(
            src_ref=src, dst_ref=dst, send_sem=send_sems.at[out_of(*out)], recv_sem=recv_sems.at[into_of(*into)],
            device_id=dev, device_id_type=MESH).start()

    def out_of(*key):
        return outs_used.setdefault(key, len(outs_used))

    def into_of(*key):
        return into_used.setdefault(key, len(into_used))

    outs_used, into_used = {}, {}

    def arrived(ref, *key):
        pltpu.make_async_remote_copy(
            src_ref=ref, dst_ref=ref, send_sem=send_sems.at[0], recv_sem=recv_sems.at[into_of(*key)],
            device_id=to_p, device_id_type=MESH).wait_recv()

    def departed(ref, *key):
        pltpu.make_async_remote_copy(
            src_ref=ref, dst_ref=ref, send_sem=send_sems.at[out_of(*key)], recv_sem=recv_sems.at[0],
            device_id=to_p, device_id_type=MESH).wait_send()

    z_copy = {0: load_z(0)}
    early = (0, 1, 3)
    turns = {}

    def turn(*key):
        turns[key] = turns.get(key, -1) + 1
        return turns[key]

    def x_turn(name):
        q, k = divmod(turn(name), ny)
        return q, (*early, 2)[k]

    stored = {}
    store_weights(in_ref, (wag_ref, wa_ref, wbg_ref, wb_ref), in_col, w_in)
    for k, ref in enumerate((wg_ref, wo_ref)):
        w_fin[k] = transposed(ref)
    out_col[...] = jnp.transpose(jnp.broadcast_to(out_ref[...].astype(F32), (lanes, hid)), (1, 0))

    def wait_stored(g):
        for copy in stored.pop(g, ()):
            copy.wait()

    def op_proj():
        g = turn("proj")
        t, h = divmod(g, groups)
        z_copy[g].wait()
        if g + 1 < crops * groups:
            z_copy[g + 1] = load_z(g + 1)
        wait_stored(g - 2)
        slot = g % 2

        def one_chunk(k, carry):
            def one_row(i, inner):
                row = k * chunk + i
                normed = normalise_row(zbuf[slot, row], in_col[...])
                prod = jnp.dot(w_in[...], normed, preferred_element_type=F32)
                mask = mask_in[t][pl.ds(h * group + row, 1), :].astype(F32)
                sa[i] = mask * jax.nn.sigmoid(prod[:hid]) * prod[hid:2 * hid]
                sb[i] = mask * jax.nn.sigmoid(prod[2 * hid:3 * hid]) * prod[3 * hid:]
                return inner

            lax.fori_loop(0, chunk, one_row, 0, unroll=min(8, chunk))
            place = pl.ds(pl.multiple_of(k * chunk, chunk), chunk)
            for e in range(0, hid, 8):
                obuf[slot, 0, e:e + 8, place, :] = jnp.transpose(sa[:, e:e + 8, :], (1, 0, 2)).astype(BF16)
                obuf[slot, 1, e:e + 8, place, :] = jnp.transpose(sb[:, e:e + 8, :], (1, 0, 2)).astype(BF16)
            return carry

        lax.fori_loop(0, group // chunk, one_chunk, 0)
        s, part = divmod(h, per_step)
        stored[g] = (
            local(obuf.at[slot, 0], a_in.at[t, :, pl.ds(h * group, group), :], "a", slot),
            local(obuf.at[slot, 1], b_in.at[t, s, :, pl.ds(part * group, group), :], "b", slot),
        )

    def a_piece(t, d):
        return a_in.at[t, pl.ds(yy[d] * cb, cb)]

    def b_piece(q, d):
        t, s = divmod(q, STEPS)
        return b_in.at[t, s, pl.ds(yy[d] * cb, cb)]

    def own_piece(q, e, d):
        if e == 0:
            return b_piece(q, 0) if d == 0 else by.at[q, d - 1]
        return bx.at[q, e - 1, d]

    def ready_rows(t, first, last):
        for h in range(first, last):
            wait_stored(t * groups + h)

    def op_a_relay():
        t = turn("a_relay")
        ready_rows(t, 0, groups)
        far = a_piece(t, 2)
        for k, dev in both_y:
            send(far.at[pl.ds(k * half, half)], a_relay.at[t, k], dev, ("ar", t), ("ar", t))

    def op_a_dir():
        t, k = divmod(turn("a_dir"), 2)
        part = pl.ds(k * half, half)
        send(a_piece(t, 1).at[part], a_all.at[t, 2, part], to_y[1], ("a", t), ("a", t))
        send(a_piece(t, 3).at[part], a_all.at[t, 0, part], to_y[3], ("a", t), ("a", t))

    def op_a_fwd():
        t = turn("a_fwd")
        arrived(a_relay.at[t], "ar", t)
        for k, dev in both_y:
            send(a_relay.at[t, k], a_all.at[t, 1, pl.ds(k * half, half)], dev, ("a", t), ("a", t))

    def op_b_start():
        q = turn("b_start")
        t, s = divmod(q, STEPS)
        ready_rows(t, s * per_step, (s + 1) * per_step)
        far = b_piece(q, 2)
        for k, dev in both_y:
            send(far.at[pl.ds(k * half, half)], b_relay.at[q, k], dev, ("br", q), ("br", q))
        send(b_piece(q, 1), by.at[q, 2], to_y[1], ("b", q), ("b", q, 3))
        send(b_piece(q, 3), by.at[q, 0], to_y[3], ("b", q), ("b", q, 1))

    def op_b_fwd():
        q = turn("b_fwd")
        arrived(b_relay.at[q], "br", q)
        for k, dev in both_y:
            send(b_relay.at[q, k], by.at[q, 1, pl.ds(k * half, half)], dev, ("b", q), ("b", q, 2))

    def cross(q, e, d):
        send(own_piece(q, e, d), bo.at[q, e, d], to_p, ("c", q), ("c", q, d))

    def op_bx():
        q, d = x_turn("bx")
        t, s = divmod(q, STEPS)
        if d == 0:
            ready_rows(t, s * per_step, (s + 1) * per_step)
        else:
            arrived(by.at[q, d - 1], "b", q, d)
        send(own_piece(q, 0, d), bx.at[q, 2, d], to_x[1], ("x", q), ("x", q, d))
        send(own_piece(q, 0, d), bx.at[q, 0, d], to_x[3], ("x", q), ("x", q, d))
        cross(q, 0, d)

    def op_xfwd():
        q, d = x_turn("xfwd")
        arrived(bx.at[q, pl.ds(0, 2), d], "x", q, d)
        for k, e in enumerate((3, 1)):
            part = pl.ds(k * half, half)
            send(bx.at[q, e - 1, d, part], bx.at[q, 1, d, part], to_x[4 - e], ("x", q), ("xf", q, d))
        for e in (3, 1):
            cross(q, e, d)

    def op_xfar():
        q, d = x_turn("xfar")
        arrived(bx.at[q, 1, d], "xf", q, d)
        cross(q, 2, d)

    loads = {}

    def load_b(q, ks):
        copies = []
        for d in ks:
            for e in range(nx):
                dst = pl.ds(pl.multiple_of(e * lanes + r * sub, sub), sub)
                copies.append(local(own_piece(q, e, d), b_v.at[d, :, dst, :], "own", e, d))
        for d in ks:
            arrived(bo.at[q, :, d], "c", q, d)
            for e in range(nx):
                dst = pl.ds(pl.multiple_of(e * lanes + (cores - 1 - r) * sub, sub), sub)
                copies.append(local(bo.at[q, e, d], b_v.at[d, :, dst, :], "other", e, d))
        return copies

    def op_load():
        q = turn("load")
        loads["b", q] = load_b(q, (0, 1))

    def op_load1():
        q = turn("load1")
        loads["b1", q] = load_b(q, (3,))

    def op_load2():
        q = turn("load2")
        loads["b2", q] = load_b(q, (2,))

    def op_load_a():
        t = turn("load_a")
        copies = [local(a_piece(t, 0), a_v.at[0], "av", 0)]
        arrived(a_all.at[t], "a", t)
        for d in (1, 3, 2):
            copies.append(local(a_all.at[t, d - 1], a_v.at[d], "av", d))
        loads["a", t] = copies

    def product(c, ks, rs):
        acc = None
        for d in ks:
            term = lax.dot_general(a_v[d, c, rs, :], b_v[d, c], (((1,), (1,)), ((), ())), preferred_element_type=F32)
            acc = term if acc is None else acc + term
        return acc

    def op_con():
        q = turn("con")
        if q % STEPS == 0:
            for copy in loads["a", q // STEPS]:
                copy.wait()
        for copy in loads["b", q]:
            copy.wait()
        slot = q % 2

        def channel(c, carry):
            acc = product(c, (0, 1), pl.ds(0, rows))
            for e in range(nx):
                o_v[slot, e, c] = acc[:, e * lanes:(e + 1) * lanes]
            return carry

        lax.fori_loop(0, cb, channel, 0)

    def op_con1():
        q = turn("con1")
        for copy in loads["b1", q]:
            copy.wait()
        slot = q % 2

        def channel(c, carry):
            acc = product(c, (3,), pl.ds(0, rows))
            for e in range(nx):
                o_v[slot, e, c] += acc[:, e * lanes:(e + 1) * lanes]
            return carry

        lax.fori_loop(0, cb, channel, 0)

    def op_con2():
        u = turn("con2")
        q, p = divmod(u, 2)
        if p == 0:
            for copy in loads["b2", q]:
                copy.wait()
        slot = q % 2
        rp = pl.ds(p * hp, hp)
        ssum[...] = jnp.zeros_like(ssum)

        def channel(c, carry):
            acc = product(c, (2,), rp)
            for e in range(nx):
                part = o_v[slot, e, c, rp, :] + acc[:, e * lanes:(e + 1) * lanes]
                o_v[slot, e, c, rp, :] = part
                ssum[e] += part
            return carry

        lax.fori_loop(0, cb, channel, 0)
        block = min(16, hr)

        def squares(k, carry, h):
            rs = pl.ds(pl.multiple_of(h * hr + k * block, block), block)
            ro = pl.ds(pl.multiple_of(p * hp + h * hr + k * block, block), block)
            rh = pl.ds(pl.multiple_of(k * block, block), block)
            for e in range(nx):
                total = ssum[e, rs, :]
                mean = total * (1.0 / cb)
                acc = jnp.zeros_like(mean)
                for c in range(cb):
                    diff = o_v[slot, e, c, ro, :] - mean
                    acc = acc + diff * diff
                st[u, e, h, 0, rh, :] = total
                st[u, e, h, 1, rh, :] = acc
            return carry

        for h in range(2):
            lax.fori_loop(0, hr // block, functools.partial(squares, h=h), 0)
        for k, dev in both_y:
            send(st.at[u, e_of[2], k], st_rx.at[u, k], dev, ("s", u), ("s", u))

    def op_rs2():
        u = turn("rs2")
        arrived(st_rx.at[u], "s", u)
        for k, d in ((0, 1), (1, 3)):
            e = e_of[d]
            got_sum, got_sq = st_rx[u, k, 0], st_rx[u, k, 1]
            my_sum, my_sq = st[u, e, k, 0], st[u, e, k, 1]
            diff = (my_sum - got_sum) * (1.0 / cb)
            st[u, e, k, 0] = my_sum + got_sum
            st[u, e, k, 1] = my_sq + got_sq + (0.5 * cb) * (diff * diff)
            send(st.at[u, e], st_in.at[u, k], to_y[d], ("s", u), ("t", u))

    def op_red():
        u = turn("red")
        arrived(st_in.at[u], "t", u)
        for h in range(2):
            parts = [(st[u, e_of[0], h, 0], st[u, e_of[0], h, 1], cb)]
            for k in range(2):
                parts.append((st_in[u, k, h, 0], st_in[u, k, h, 1], 2 * cb if k == h else cb))
            mean = (parts[0][0] + parts[1][0] + parts[2][0]) * (1.0 / hid)
            m2 = jnp.zeros_like(mean)
            for total, sq, n in parts:
                diff = total * (1.0 / n) - mean
                m2 = m2 + sq + n * (diff * diff)
            mr[u, h, 0] = mean
            mr[u, h, 1] = lax.rsqrt(m2 * (1.0 / hid) + EPS)
        send(mr.at[u], mr_in.at[u, 2], to_y[1], ("m", u), ("m", u))
        send(mr.at[u], mr_in.at[u, 0], to_y[3], ("m", u), ("m", u))

    def apply_norm(u, d):
        q, p = divmod(u, 2)
        e = e_of[d]
        for h in range(2):
            src = mr.at[u, h] if d == 0 else mr_in.at[u, d - 1, h]
            mean, rstd = src[0], src[1]

            def channel(c, carry, mean=mean, rstd=rstd, h=h):
                scale = out_col[pl.ds(y * cb + c, 1), :]
                value = (o_v[q % 2, e, c, pl.ds(p * hp + h * hr, hr), :] - mean) * rstd * scale
                nv[u, d, c, pl.ds(h * hr, hr), :] = value.astype(BF16)
                return carry

            lax.fori_loop(0, cb, channel, 0)

    def n_place(u, owner, *part):
        q, p = divmod(u, 2)
        return n_out.at[q, owner, *(part or (slice(None),)), pl.ds(p * hp, hp), :]

    keep = {}

    def op_ag2():
        u = turn("ag2")
        arrived(mr_in.at[u, pl.ds(0, 2)], "m", u)
        send(mr_in.at[u, 2, 0], mr_in.at[u, 1, 0], to_y[1], ("m", u), ("mf", u))
        send(mr_in.at[u, 0, 1], mr_in.at[u, 1, 1], to_y[3], ("m", u), ("mf", u))
        for d in (1, 3, 0):
            apply_norm(u, d)
        send(nv.at[u, 1], n_place(u, y), to_y[1], ("n", u), ("n", u))
        send(nv.at[u, 3], n_place(u, y), to_y[3], ("n", u), ("n", u))
        keep[u] = local(nv.at[u, 0], n_place(u, y), "keep", u)

    def op_norm():
        u = turn("norm")
        arrived(mr_in.at[u, 1], "mf", u)
        apply_norm(u, 2)
        for k, dev in both_y:
            send(nv.at[u, 2, pl.ds(k * half, half)], n_relay.at[u, k], dev, ("nr", u), ("nr", u))

    def op_nfwd():
        u = turn("nfwd")
        arrived(n_relay.at[u], "nr", u)
        for k, dev in both_y:
            owner = yy[3] if k == 0 else yy[1]
            send(n_relay.at[u, k], n_place(u, owner, pl.ds(k * half, half)), dev, ("n", u), ("n", u))

    def op_nwait():
        u = turn("nwait")
        arrived(nv.at[u, pl.ds(0, 3)], "n", u)
        keep[u].wait()

    def op_fin():
        f = turn("fin")
        t, h = divmod(f, groups)
        place = pl.ds(h * group, group)
        wait_stored(crops * groups - 2)
        wait_stored(crops * groups - 1)
        copies = [local(z_in[t].at[place], zbuf.at[0], "z", 0)]
        for s in range(STEPS):
            copies.append(local(n_out.at[t * STEPS + s, :, :, place, :], nbuf.at[s], "n", s))
        for copy in copies:
            copy.wait()
        if f:
            keep["f"].wait()

        def one_chunk(k, carry):
            at = pl.ds(pl.multiple_of(k * chunk, chunk), chunk)
            for blk in range(ny):
                for e in range(0, cb, 8):
                    merge_lanes(sa, blk * cb + e, [nbuf[s, blk, e:e + 8, at, :] for s in range(STEPS)], cores)

            def one_row(i, inner):
                row = k * chunk + i
                fbuf[row] = finish_row(zbuf[0, row], sa[i], in_col[...], w_fin[0], w_fin[1])
                return inner

            lax.fori_loop(0, chunk, one_row, 0, unroll=min(8, chunk))
            return carry

        lax.fori_loop(0, group // chunk, one_chunk, 0)
        keep["f"] = local(fbuf, done.at[pl.ds(f * group, group)], "f")

    table = dict(proj=op_proj, a_relay=op_a_relay, a_dir=op_a_dir, a_fwd=op_a_fwd, b_start=op_b_start, b_fwd=op_b_fwd,
                 bx=op_bx, xfwd=op_xfwd, xfar=op_xfar, load=op_load, load_a=op_load_a, load1=op_load1, load2=op_load2, con1=op_con1, con=op_con, con2=op_con2, rs2=op_rs2,
                 red=op_red, ag2=op_ag2, norm=op_norm, nfwd=op_nfwd, nwait=op_nwait, fin=op_fin)
    for name in ORDER:
        table[name]()
    keep["f"].wait()
    for t in range(crops):
        departed(a_relay.at[t], "ar", t)
        departed(a_all.at[t], "a", t)
    for q in range(crops * STEPS):
        departed(b_relay.at[q], "br", q)
        departed(by.at[q], "b", q)
        departed(bx.at[q], "x", q)
        departed(bo.at[q], "c", q)
    for u in range(2 * crops * STEPS):
        departed(mr_in.at[u], "s", u)
        departed(mr_in.at[u], "m", u)
        departed(n_relay.at[u], "nr", u)
        departed(nv.at[u, pl.ds(0, 3)], "n", u)


def exchange(crops, masks, rows_in, ny, nx, cores):
    rows, ch, cols = crops[0].shape
    hid = rows_in[-1].shape[1]
    cb = hid // ny
    sub = rows // STEPS
    lanes = cores * sub
    hp = rows // 2
    hr = hp // 2
    q = 2 * STEPS
    u = 2 * q
    group = rows // 4
    chunk = min(ROWS, group)
    any_spec = pl.BlockSpec(memory_space=pl.ANY)
    vmem = pl.BlockSpec(memory_space=pltpu.VMEM)

    def hbm(*shape):
        return jax.ShapeDtypeStruct(shape, BF16)

    sends = 2 * 2 + q * 4 + u * 4
    arrivals = 2 * 2 + q * (4 + 3 * ny) + u * 6
    locals_ = 6 + 2 * nx * ny + ny + u + STEPS + 1
    outs = pl.pallas_call(
        functools.partial(exchange_kernel, ny, nx, cores),
        in_specs=[any_spec] * 2 + [vmem] * (2 + len(rows_in)),
        out_specs=[any_spec] * 11,
        out_shape=[
            hbm(rows, ch, cols),
            hbm(q, ny, cb, rows, lanes),
            hbm(2, ny - 1, cb, rows, cols),
            hbm(2, 2, cb // 2, rows, cols),
            hbm(q, ny - 1, cb, sub, cols),
            hbm(q, 2, cb // 2, sub, cols),
            hbm(q, nx - 1, ny, cb, sub, cols),
            hbm(q, nx, ny, cb, sub, cols),
            hbm(u, 2, cb // 2, hp, lanes),
            hbm(2, hid, rows, cols),
            hbm(2, STEPS, hid, sub, cols),
        ],
        scratch_shapes=[
            pltpu.VMEM((ny, cb, rows, cols), BF16),
            pltpu.VMEM((ny, cb, nx * lanes, cols), BF16),
            pltpu.VMEM((2, nx, cb, rows, lanes), F32),
            pltpu.VMEM((nx, hp, lanes), F32),
            pltpu.VMEM((u, nx, 2, 2, hr, lanes), F32),
            pltpu.VMEM((u, 2, 2, hr, lanes), F32),
            pltpu.VMEM((u, 2, 2, 2, hr, lanes), F32),
            pltpu.VMEM((u, 2, 2, hr, lanes), F32),
            pltpu.VMEM((u, ny - 1, 2, 2, hr, lanes), F32),
            pltpu.VMEM((u, ny, cb, hp, lanes), BF16),
            pltpu.VMEM((2, group, ch, cols), BF16),
            pltpu.VMEM((chunk, hid, cols), F32),
            pltpu.VMEM((chunk, hid, cols), F32),
            pltpu.VMEM((2, 2, hid, group, cols), BF16),
            pltpu.VMEM((STEPS, ny, cb, group, lanes), BF16),
            pltpu.VMEM((group, ch, cols), BF16),
            pltpu.VMEM((4 * hid, ch), BF16),
            pltpu.VMEM((2, ch, hid), BF16),
            pltpu.VMEM((ch, cols), F32),
            pltpu.VMEM((hid, lanes), F32),
            pltpu.SemaphoreType.DMA((sends,)),
            pltpu.SemaphoreType.DMA((arrivals,)),
            pltpu.SemaphoreType.DMA((locals_,)),
        ],
        compiler_params=pltpu.CompilerParams(collective_id=0, has_side_effects=True, vmem_limit_bytes=VMEM_LIMIT),
        cost_estimate=pl.CostEstimate(flops=4 * rows * cols * hid * nx * cols, bytes_accessed=200000000, transcendentals=0),
        name="exchange",
    )(*crops, *masks, *rows_in)
    return outs[0], outs[1].reshape(q, hid, rows, lanes)


def solution(mesh):
    row_count = mesh.shape['row']
    col_count = mesh.shape['col']
    cores = row_count // col_count
    nx = row_count // cores
    pair_spec = P(('batch', 'row'), 'col', None)
    mask_spec = P(('batch', 'row'), 'col')
    replicated = P()

    def device_fn(z_one, z_two, mask_one, mask_two, ln_in_scale, w_a, w_a_gate, w_b, w_b_gate, w_gate, w_out, ln_out_scale):
        in_row = ln_in_scale[None, :]
        crops = [jnp.transpose(z, (0, 2, 1)) for z in (z_one, z_two)]
        done, n_all = exchange(crops, (mask_one, mask_two),
                                (in_row, w_a_gate, w_a, w_b_gate, w_b, w_gate, w_out, ln_out_scale[None, :]),
                                col_count, nx, cores)
        outs = finish(crops[1], done, n_all, cores, in_row, w_gate, w_out)
        return tuple(jnp.transpose(o, (0, 2, 1)) for o in outs)

    return jax.shard_map(
        device_fn,
        mesh=mesh,
        in_specs=(pair_spec, pair_spec, mask_spec, mask_spec) + (replicated,) * 8,
        out_specs=(pair_spec, pair_spec),
        check_vma=False,
    )
```
